128 devices in a mesh: gx: 8 (over z, y_hi), gy: 16 (over y_lo, x, core).
Axes of the slice: x: 4, y: 4 (y_hi: 2, y_lo: 2; y = y_hi * 2 + y_lo), z: 4, core: 2. Of those that a mesh axis runs over, the one named last changes fastest.
Arguments:
- spectrum: float32 [2, 1024, 16384], P(None, ('gx', 'gy')), may hold values from -6 to 6
- parameters: float32 [2], replicated, may hold values from -1.5 to 1.5
Outputs:
- advanced: float32 [2, 1024, 16384], P(None, ('gx', 'gy'))
The draws below stay inside these ranges and needn't reach their ends.
All inputs are finite; a program needn't handle non-finite values.
Results may differ from the reference program's by a relative error of at most 0.0003.
Values sent between devices are 32-bit elements; how exact they have to be, the bound alone decides.
A program may use at most 128 MiB of HBM per device.

```python
import math
import jax
import jax.numpy as jnp

COLS = 16384
STEPS = 1
ROWS = 1024


def levels(own_key, shape, pieces, least, largest):
    factor_of, own = 1.0, jax.random.fold_in(own_key, 6)
    for dim, parts in pieces:
        draws = jnp.exp(jax.random.uniform(jax.random.fold_in(own, dim), (parts,), jnp.float32, least / len(pieces), largest / len(pieces)))
        factor_of = factor_of * jnp.repeat(draws, shape[dim] // parts).reshape([-1 if axis == dim else 1 for axis in range(len(shape))])
    return factor_of


def scatter_about(own_key, extent, deviation, limit, pieces=(), held_as=jnp.bfloat16):
    factor_of = levels(own_key, extent, pieces, -0.22, 0.18) if pieces else 1.0
    array = jax.random.normal(own_key, extent, jnp.float32) * deviation * factor_of
    return jnp.minimum(jnp.maximum(array, -limit), limit).astype(held_as)


def setup_inputs(seed: int = 0) -> dict:
    seeds = jax.random.split(jax.random.key(seed), 3)
    return {
        "spectrum": scatter_about(seeds[0], (2, ROWS, COLS), 1.0, 6.0, ((1, 128),), jnp.float32),
        "parameters": jnp.clip(jax.random.uniform(seeds[1], (2,), jnp.float32, -1.5, 1.5), -1.5, 1.5),
    }


time_step = 0.1
spacing = 0.25


def phi_series(zeta):
    result = []
    for phi_order in (1, 2, 3):
        running = jnp.full_like(zeta, 1.0 / math.factorial(14 + phi_order))
        for degree in range(13, -1, -1):
            running = running * zeta + 1.0 / math.factorial(degree + phi_order)
        result.append(running)
    return result


def phi_values(zeta):
    inside = zeta.real * zeta.real + zeta.imag * zeta.imag < 1.0
    guarded = jnp.where(inside, jnp.ones_like(zeta), zeta)
    series = phi_series(zeta)
    phi_one = (jnp.exp(guarded) - 1.0) / guarded
    phi_two = (phi_one - 1.0) / guarded
    phi_three = (phi_two - 0.5) / guarded
    direct = [phi_one, phi_two, phi_three]
    return [jnp.where(inside, series[index], direct[index]) for index in range(3)]


def reference(spectrum, parameters):
    rows_all = spectrum.shape[1]
    columns = spectrum.shape[2]
    modes_total = rows_all * columns
    current = (spectrum[0] + 1j * spectrum[1]).reshape(modes_total)
    mode_index = jnp.arange(modes_total, dtype=jnp.int32)
    signed = jnp.where(mode_index < modes_total // 2, mode_index, mode_index - modes_total).astype(spectrum.dtype)
    wavenum = signed * (2.0 * math.pi / (modes_total * spacing))
    wave_square = wavenum * wavenum
    dispersion = parameters[0]
    cubic_twist = parameters[1]
    zeta = time_step * (1.0 - wave_square) - 1j * (time_step * dispersion * wave_square)
    phi_one, phi_two, phi_three = phi_values(zeta)
    half_weight = 0.5 * time_step * phi_values(zeta / 2.0)[0]
    decay_full = jnp.exp(zeta)
    decay_half = jnp.exp(zeta / 2.0)
    weight_one = time_step * (phi_one - 3.0 * phi_two + 4.0 * phi_three)
    weight_two = time_step * (phi_two - 2.0 * phi_three)
    weight_three = time_step * (4.0 * phi_three - phi_two)

    def nonlinear(spectral):
        physical = jnp.fft.ifft(spectral, norm="ortho")
        magnitude = physical.real * physical.real + physical.imag * physical.imag
        cubic = -(1.0 + 1j * cubic_twist) * magnitude * physical
        return jnp.fft.fft(cubic, norm="ortho")

    for repeat in range(STEPS):
        start_term = nonlinear(current)
        inner_one = decay_half * current + half_weight * start_term
        one_term = nonlinear(inner_one)
        inner_two = decay_half * current + half_weight * one_term
        two_term = nonlinear(inner_two)
        inner_three = decay_half * inner_one + half_weight * (2.0 * two_term - start_term)
        three_term = nonlinear(inner_three)
        current = (decay_full * current + weight_one * start_term
                   + 2.0 * weight_two * (one_term + two_term) + weight_three * three_term)
    return jnp.stack([current.real, current.imag]).reshape(2, rows_all, columns)
```

```python
import math

import jax
import jax.numpy as jnp
from jax import lax
from jax.experimental import pallas as pl
from jax.experimental.pallas import tpu as pltpu
from jax.sharding import PartitionSpec as P

time_step = 0.1
spacing = 0.25
highest = lax.Precision.HIGHEST


MESH = pl.DeviceIdType.MESH


def spread(j):
    return 2 + j - (j // 2) * (2 * j - 1)


def partner(me, i):
    z = lax.rem(me // 32 + spread(i // 32), 4)
    y = lax.rem(me // 8 + spread(lax.rem(i // 8, 4)), 4)
    x = lax.rem(me // 2 + spread(lax.rem(i // 2, 4)), 4)
    core = lax.rem(me + 1 + lax.rem(i, 2), 2)
    return z * 32 + y * 8 + x * 2 + core


def target(device):
    return {"gx": device // 16, "gy": lax.rem(device, 16)}


def exchange_kernel(x_ref, o_ref, send_sem, recv_sem):
    me = lax.axis_index("gx") * 16 + lax.axis_index("gy")
    barrier = pltpu.get_barrier_semaphore()

    def greet(i, carry):
        pl.semaphore_signal(barrier, 1, device_id=target(partner(me, i)), device_id_type=MESH)
        return carry

    lax.fori_loop(0, 127, greet, 0)
    pl.semaphore_wait(barrier, 127)

    def send(i, carry):
        other = partner(me, i)
        pltpu.make_async_remote_copy(
            x_ref.at[other], o_ref.at[me], send_sem, recv_sem,
            device_id=target(other), device_id_type=MESH,
        ).start()
        return carry

    lax.fori_loop(0, 127, send, 0)
    o_ref[me] = x_ref[me]
    most = o_ref.at[pl.ds(0, 127)]
    pltpu.make_async_copy(most, most, recv_sem).wait()
    pltpu.make_async_copy(most, most, send_sem).wait()


def exchange(blocks):
    shape = blocks.shape
    return pl.pallas_call(
        exchange_kernel,
        name="exchange",
        out_shape=jax.ShapeDtypeStruct(shape, jnp.float32),
        in_specs=[pl.BlockSpec(memory_space=pltpu.VMEM)],
        out_specs=pl.BlockSpec(memory_space=pltpu.VMEM),
        scratch_shapes=[pltpu.SemaphoreType.DMA, pltpu.SemaphoreType.DMA],
        compiler_params=pltpu.CompilerParams(collective_id=0, has_side_effects=True),
    )(blocks)


def to_rows(whole):
    parts, rows, columns = whole.shape
    blocks = whole.reshape(2, 128, 8, 128).transpose(1, 0, 2, 3)
    return exchange(blocks.reshape(128, 16, 128)).reshape(128, 2, 8, 128).transpose(1, 2, 0, 3)


def to_columns(whole):
    blocks = whole.reshape(2, 8, 128, 128).transpose(2, 0, 1, 3)
    return exchange(blocks.reshape(128, 16, 128)).reshape(128, 2, 8, 128).transpose(1, 0, 2, 3)


def angle_tables(rows_idx, cols_idx, length, orient):
    product = rows_idx[:, None] * cols_idx[None, :] % length
    angles = product.astype(jnp.float32) * (2.0 * math.pi / length)
    return (jnp.cos(angles), orient * jnp.sin(angles))


def dft_tables(length, orient):
    counter = jnp.arange(length, dtype=jnp.int32)
    return angle_tables(counter, counter, length, orient)


def complex_section(formula, tables, parts):
    cosine, sine_part = tables
    former, latter = parts
    real_out = jnp.einsum(formula, cosine, former, precision=highest) - jnp.einsum(
        formula, sine_part, latter, precision=highest
    )
    imag_out = jnp.einsum(formula, cosine, latter, precision=highest) + jnp.einsum(
        formula, sine_part, former, precision=highest
    )
    return (real_out, imag_out)


def complex_times(factor, operand):
    return (
        factor[0] * operand[0] - factor[1] * operand[1],
        factor[0] * operand[1] + factor[1] * operand[0],
    )


def complex_over(operand, factor):
    denominator = factor[0] * factor[0] + factor[1] * factor[1]
    return (
        (operand[0] * factor[0] + operand[1] * factor[1]) / denominator,
        (operand[1] * factor[0] - operand[0] * factor[1]) / denominator,
    )


def radix_split(length):
    return (128, length // 128)


def dft_first(parts, orient):
    length, breadth = parts[0].shape
    radix_size, remain = radix_split(length)
    shaped = (
        parts[0].reshape(radix_size, remain, breadth),
        parts[1].reshape(radix_size, remain, breadth),
    )
    sectioned = complex_section("pq,qnk->pnk", dft_tables(radix_size, orient), shaped)
    turns = angle_tables(
        jnp.arange(radix_size, dtype=jnp.int32), jnp.arange(remain, dtype=jnp.int32), length, orient
    )
    turned = complex_times((turns[0][:, :, None], turns[1][:, :, None]), sectioned)
    finished = complex_section("rn,pnk->rpk", dft_tables(remain, orient), turned)
    return (finished[0].reshape(length, breadth), finished[1].reshape(length, breadth))


def dft_last(parts, orient):
    batch_rows, length = parts[0].shape
    radix_size, remain = radix_split(length)
    shaped = (
        parts[0].reshape(batch_rows, radix_size, remain),
        parts[1].reshape(batch_rows, radix_size, remain),
    )
    sectioned = complex_section("pq,bqn->bpn", dft_tables(radix_size, orient), shaped)
    turns = angle_tables(
        jnp.arange(radix_size, dtype=jnp.int32), jnp.arange(remain, dtype=jnp.int32), length, orient
    )
    turned = complex_times((turns[0][None], turns[1][None]), sectioned)
    finished = complex_section("rn,bpn->brp", dft_tables(remain, orient), turned)
    return (finished[0].reshape(batch_rows, length), finished[1].reshape(batch_rows, length))


def phi_values(zeta_real, zeta_imag):
    inside = zeta_real * zeta_real + zeta_imag * zeta_imag < 1.0
    guarded = (jnp.where(inside, 1.0, zeta_real), jnp.where(inside, 0.0, zeta_imag))
    growth = jnp.exp(guarded[0])
    phi_one = complex_over(
        (growth * jnp.cos(guarded[1]) - 1.0, growth * jnp.sin(guarded[1])), guarded
    )
    phi_two = complex_over((phi_one[0] - 1.0, phi_one[1]), guarded)
    phi_three = complex_over((phi_two[0] - 0.5, phi_two[1]), guarded)
    direct = [phi_one, phi_two, phi_three]
    result = []
    for phi_order in (1, 2, 3):
        running = (
            jnp.full_like(zeta_real, 1.0 / math.factorial(14 + phi_order)),
            jnp.zeros_like(zeta_real),
        )
        for degree in range(13, -1, -1):
            running = complex_times(running, (zeta_real, zeta_imag))
            running = (running[0] + 1.0 / math.factorial(degree + phi_order), running[1])
        chosen = direct[phi_order - 1]
        result.append(
            jnp.stack(
                [jnp.where(inside, running[0], chosen[0]), jnp.where(inside, running[1], chosen[1])]
            )
        )
    return result


def coefficients(mode_index, modes_total, dispersion):
    signed = jnp.where(mode_index < modes_total // 2, mode_index, mode_index - modes_total).astype(
        jnp.float32
    )
    wavenum = signed * (2.0 * math.pi / (modes_total * spacing))
    wave_square = wavenum * wavenum
    zeta_real = time_step * (1.0 - wave_square)
    zeta_imag = -(time_step * dispersion * wave_square)
    phi_one, phi_two, phi_three = phi_values(zeta_real, zeta_imag)
    half_weight = 0.5 * time_step * phi_values(0.5 * zeta_real, 0.5 * zeta_imag)[0]
    growth = jnp.exp(zeta_real)
    decay_full = jnp.stack([growth * jnp.cos(zeta_imag), growth * jnp.sin(zeta_imag)])
    halfway = jnp.exp(0.5 * zeta_real)
    decay_half = jnp.stack([halfway * jnp.cos(0.5 * zeta_imag), halfway * jnp.sin(0.5 * zeta_imag)])
    weight_one = time_step * (phi_one - 3.0 * phi_two + 4.0 * phi_three)
    weight_two = time_step * (phi_two - 2.0 * phi_three)
    weight_three = time_step * (4.0 * phi_three - phi_two)
    return (decay_full, decay_half, half_weight, weight_one, weight_two, weight_three)


def scaled_by(factor, operand):
    return jnp.stack(complex_times((factor[0], factor[1]), (operand[0], operand[1])))


def advance(current, nonlinear, weights):
    decay_full, decay_half, half_weight, weight_one, weight_two, weight_three = weights
    start_term = nonlinear(current)
    inner_one = scaled_by(decay_half, current) + scaled_by(half_weight, start_term)
    one_term = nonlinear(inner_one)
    inner_two = scaled_by(decay_half, current) + scaled_by(half_weight, one_term)
    two_term = nonlinear(inner_two)
    inner_three = scaled_by(decay_half, inner_one) + scaled_by(
        half_weight, 2.0 * two_term - start_term
    )
    three_term = nonlinear(inner_three)
    return (
        scaled_by(decay_full, current)
        + scaled_by(weight_one, start_term)
        + 2.0 * scaled_by(weight_two, one_term + two_term)
        + scaled_by(weight_three, three_term)
    )


def local(spectrum, parameters):
    devices = lax.axis_size(("gx", "gy"))
    device = lax.axis_index(("gx", "gy"))
    row_shard = spectrum.shape[1]
    columns = spectrum.shape[2]
    all_rows = row_shard * devices
    col_shard = columns // devices
    modes_total = all_rows * columns
    dispersion = parameters[0]
    cubic_twist = parameters[1]
    norm_scale = 1.0 / math.sqrt(modes_total)
    all_index = jnp.arange(all_rows, dtype=jnp.int32)
    all_cols = jnp.arange(columns, dtype=jnp.int32)
    row_index = device * row_shard + jnp.arange(row_shard, dtype=jnp.int32)
    col_index = device * col_shard + jnp.arange(col_shard, dtype=jnp.int32)
    inverse_turn = angle_tables(all_index, col_index, modes_total, 1.0)
    forward_turn = angle_tables(row_index, all_cols, modes_total, -1.0)

    def unfold_local(spectral):
        return jnp.stack(dft_first((spectral[0], spectral[1]), 1.0))

    def physics(received):
        physical = dft_last((received[0, 0], received[1, 0]), 1.0)
        phys_real = physical[0] * norm_scale
        phys_imag = physical[1] * norm_scale
        magnitude = phys_real * phys_real + phys_imag * phys_imag
        cubic_real = -magnitude * (phys_real - cubic_twist * phys_imag)
        cubic_imag = -magnitude * (phys_imag + cubic_twist * phys_real)
        return jnp.stack(dft_last((cubic_real, cubic_imag), -1.0))[:, None]

    def finish(received):
        spectral = dft_first((received[0, :, 0], received[1, :, 0]), -1.0)
        return jnp.stack([spectral[0] * norm_scale, spectral[1] * norm_scale])[:, :, None]

    def physical_pass(opened):
        turned = jnp.stack(complex_times(inverse_turn, (opened[0], opened[1])))
        physical = physics(
            to_rows(turned).reshape(2, 1, row_shard, columns)
        )
        turned_back = jnp.stack(complex_times(forward_turn, (physical[0, 0], physical[1, 0])))
        spectral = finish(
            to_columns(turned_back).reshape(2, all_rows, 1, col_shard)
        )
        return spectral.reshape(2, all_rows, col_shard)

    weights = coefficients(
        all_index[:, None] * columns + col_index[None, :], modes_total, dispersion
    )

    def nonlinear_columns(spectral):
        return physical_pass(unfold_local(spectral))

    entered = to_columns(spectrum)
    current = entered.reshape(2, all_rows, col_shard)
    current = advance(current, nonlinear_columns, weights)
    leaving = to_rows(current)
    return leaving.reshape(2, row_shard, columns)


def solution(mesh):
    return jax.shard_map(
        local,
        mesh=mesh,
        in_specs=(P(None, ("gx", "gy"), None), P()),
        out_specs=P(None, ("gx", "gy"), None),
        check_vma=False,
    )
```

```python
import itertools
import math
import random

import jax
import jax.numpy as jnp
import numpy as np
from jax import lax
from jax.experimental import pallas as pl
from jax.experimental.pallas import tpu as pltpu
from jax.sharding import PartitionSpec as P

MESH = pl.DeviceIdType.MESH
F32 = jnp.float32
BF16 = jnp.bfloat16

time_step = 0.1
spacing = 0.25
DEVICES = 128
ROWS = 1024
COLS = 16384
TOTAL = ROWS * COLS
NORM = 1.0 / math.sqrt(TOTAL)
LANES = 128

FULL, HALF, QUARTER, FIRST, SECOND, THIRD = 0, 2, 1, 3, 4, 5
WEIGHT, LAST = 0, 1


def offsets():
    every = [o for o in itertools.product(range(4), range(4), range(4), range(2)) if any(o)]
    random.Random(0).shuffle(every)
    return sorted(every, key=lambda o: -sum(min(v, 4 - v) for v in o[:3]))


OTHERS = offsets()


def split_host(table):
    high = table.astype(np.float32).astype(jnp.bfloat16)
    low = (table - high.astype(np.float64)).astype(np.float32).astype(jnp.bfloat16)
    return high, low


def left_table(sign, scale):
    index = np.arange(128)
    angle = 2.0 * np.pi * (np.outer(index, index) % 128) / 128
    cosine, sine = np.cos(angle) * scale, sign * np.sin(angle) * scale
    high, low = split_host(np.block([[cosine, -sine], [sine, cosine]]))
    return np.concatenate([high, high, low], axis=1)


def right_table(sign, scale):
    index = np.arange(128)
    angle = 2.0 * np.pi * (np.outer(index, index) % 128) / 128
    cosine, sine = np.cos(angle) * scale, sign * np.sin(angle) * scale
    high, low = split_host(np.block([[cosine, sine], [-sine, cosine]]))
    return np.concatenate([high, high, low], axis=0)


def inner_turns():
    index = np.arange(128)
    angle = 2.0 * np.pi * np.outer(index, index) / COLS
    return np.stack([np.cos(angle), np.sin(angle)]).astype(np.float32)


def times(a, b):
    return a[0] * b[0] - a[1] * b[1], a[0] * b[1] + a[1] * b[0]


def times_conj(a, b):
    return a[0] * b[0] + a[1] * b[1], a[1] * b[0] - a[0] * b[1]


def plus(a, b):
    return a[0] + b[0], a[1] + b[1]


def minus(a, b):
    return a[0] - b[0], a[1] - b[1]


def turn(a, sign):
    return (-a[1], a[0]) if sign > 0 else (a[1], -a[0])


def four(x, sign):
    s02, d02 = plus(x[0], x[2]), minus(x[0], x[2])
    s13, d13 = plus(x[1], x[3]), turn(minus(x[1], x[3]), sign)
    return [plus(s02, s13), plus(d02, d13), minus(s02, s13), minus(d02, d13)]


def eight(x, sign):
    even, odd = four(x[0::2], sign), four(x[1::2], sign)
    half = math.sqrt(0.5)
    odd[1] = plus(odd[1], turn(odd[1], sign))
    odd[1] = (odd[1][0] * half, odd[1][1] * half)
    odd[2] = turn(odd[2], sign)
    odd[3] = minus(turn(odd[3], sign), odd[3])
    odd[3] = (odd[3][0] * half, odd[3][1] * half)
    return [plus(even[k], odd[k]) for k in range(4)] + [minus(even[k], odd[k]) for k in range(4)]


def cos_sin_quarter(quarters):
    whole = jnp.floor(quarters + 0.5)
    return cos_sin_near((quarters - whole) * (math.pi / 2), whole)


def cos_sin_near(x, whole):
    square = x * x
    sine = 1.0 / 362880.0
    for factor in (-1.0 / 5040.0, 1.0 / 120.0, -1.0 / 6.0, 1.0):
        sine = sine * square + factor
    sine = sine * x
    cosine = -1.0 / 3628800.0
    for factor in (1.0 / 40320.0, -1.0 / 720.0, 1.0 / 24.0, -0.5, 1.0):
        cosine = cosine * square + factor
    quadrant = whole.astype(jnp.int32) & 3
    swap = (quadrant & 1) == 1
    first = jnp.where(swap, sine, cosine)
    second = jnp.where(swap, cosine, sine)
    first = jnp.where((quadrant == 1) | (quadrant == 2), -first, first)
    second = jnp.where(quadrant >= 2, -second, second)
    return first, second


def cos_sin(x):
    whole = jnp.floor(x * (2.0 / math.pi) + 0.5)
    near = x - whole * 1.5703125
    near = near - whole * 4.837512969970703e-4
    near = near - whole * 7.549789948768648e-8
    return cos_sin_near(near, whole)


def series(z, order):
    real = jnp.full_like(z[0], 1.0 / math.factorial(14 + order))
    imag = jnp.zeros_like(z[0])
    for degree in range(13, -1, -1):
        real, imag = times((real, imag), z)
        real = real + 1.0 / math.factorial(degree + order)
    return real, imag


def over(z):
    scale = 1.0 / (z[0] * z[0] + z[1] * z[1])
    return z[0] * scale, -z[1] * scale


def pick(inside, a, b):
    return jnp.where(inside, a[0], b[0]), jnp.where(inside, a[1], b[1])


def coefficient_block(rows, columns, dispersion):
    mode = rows * COLS + columns
    signed = jnp.where(mode < TOTAL // 2, mode, mode - TOTAL).astype(F32)
    wavenum = signed * (2.0 * math.pi / (TOTAL * spacing))
    square = wavenum * wavenum
    z = time_step * (1.0 - square), -(time_step * dispersion * square)
    half = 0.5 * z[0], 0.5 * z[1]
    growth = jnp.exp(half[0])
    cosine, sine = cos_sin(half[1])
    decay_half = growth * cosine, growth * sine
    decay_full = times(decay_half, decay_half)

    inside = z[0] * z[0] + z[1] * z[1] < 1.0
    inverse = over((jnp.where(inside, 1.0, z[0]), jnp.where(inside, 0.0, z[1])))
    direct_one = times((decay_full[0] - 1.0, decay_full[1]), inverse)
    direct_two = times((direct_one[0] - 1.0, direct_one[1]), inverse)
    direct_three = times((direct_two[0] - 0.5, direct_two[1]), inverse)
    near_three = series(z, 3)
    near_two = times(near_three, z)
    near_two = near_two[0] + 0.5, near_two[1]
    near_one = times(near_two, z)
    near_one = near_one[0] + 1.0, near_one[1]
    one = pick(inside, near_one, direct_one)
    two = pick(inside, near_two, direct_two)
    three = pick(inside, near_three, direct_three)

    inside = half[0] * half[0] + half[1] * half[1] < 1.0
    inverse = over((jnp.where(inside, 1.0, half[0]), jnp.where(inside, 0.0, half[1])))
    direct = times((decay_half[0] - 1.0, decay_half[1]), inverse)
    half_one = pick(inside, series(half, 1), direct)

    return {
        FULL: decay_full,
        QUARTER: decay_half,
        HALF: tuple(0.5 * time_step * p for p in half_one),
        FIRST: tuple(time_step * (p - 3.0 * q + 4.0 * r) for p, q, r in zip(one, two, three)),
        SECOND: tuple(2.0 * time_step * (q - 2.0 * r) for q, r in zip(two, three)),
        THIRD: tuple(time_step * (4.0 * r - q) for q, r in zip(two, three)),
    }


def split(x):
    high = x.astype(BF16)
    return high, (x - high.astype(F32)).astype(BF16)


def from_left(table_ref, real, imag):
    high, low = split(jnp.concatenate([real, imag], axis=0))
    stacked = jnp.concatenate([high, low, high], axis=0)
    out = jnp.dot(table_ref[...], stacked, preferred_element_type=F32)
    return out[:128], out[128:]


def from_right(table_ref, real, imag):
    high, low = split(jnp.concatenate([real, imag], axis=1))
    stacked = jnp.concatenate([high, low, high], axis=1)
    out = jnp.dot(stacked, table_ref[...], preferred_element_type=F32)
    return out[:, :128], out[:, 128:]


def kernel(
    par, x_hbm, li_hbm, lf_hbm, ri_hbm, rf_hbm, tw_hbm,
    o_hbm,
    xin, li, lf, ri, rf, tw, turns, ticks, coef, w, nbuf, lin, tmp, mid,
    sb1, rb1, sb2, rb2,
    load_sem, enter_sem, leave_sem, s1, r1, s2, r2,
):
    gx, gy = lax.axis_index("gx"), lax.axis_index("gy")
    me = gx * 16 + gy
    z, y, x, core = me // 32, lax.rem(me // 8, 4), lax.rem(me // 2, 4), lax.rem(me, 2)
    zs = [lax.rem(z + i, 4) * 2 for i in range(4)]
    yh = [lax.rem(y + i, 4) // 2 for i in range(4)]
    yl = [lax.rem(lax.rem(y + i, 4), 2) * 8 for i in range(4)]
    xs = [lax.rem(x + i, 4) * 2 for i in range(4)]
    cs = [core, 1 - core]

    def partners():
        for oz, oy, ox, oc in OTHERS:
            tx = zs[oz] + yh[oy]
            ty = yl[oy] + xs[ox] + cs[oc]
            yield tx * 16 + ty, {"gx": tx, "gy": ty}

    def tile(index):
        return pl.ds(pl.multiple_of(index * 8, 8), 8)

    def band(index):
        return pl.ds(pl.multiple_of(index * LANES, LANES), LANES)

    loads = [
        pltpu.make_async_copy(source, target, load_sem.at[i])
        for i, (source, target) in enumerate(
            [(x_hbm, xin), (li_hbm, li), (lf_hbm, lf), (ri_hbm, ri), (rf_hbm, rf), (tw_hbm, tw)]
        )
    ]
    for load in loads:
        load.start()

    barrier = pltpu.get_barrier_semaphore()
    for _, there in partners():
        pl.semaphore_signal(barrier, 1, device_id=there, device_id_type=MESH)
    pl.semaphore_wait(barrier, DEVICES - 1)

    loads[0].wait()
    for part in range(2):
        for other, there in partners():
            pltpu.make_async_remote_copy(
                xin.at[part, :, band(other)], w.at[part, tile(me)],
                enter_sem.at[0], enter_sem.at[1], device_id=there, device_id_type=MESH,
            ).start()
        w[part, tile(me), :] = xin[part, :, band(me)]

    dispersion, twist = par[0], par[1]
    lane = lax.broadcasted_iota(jnp.int32, (8, LANES), 1)
    sub = lax.broadcasted_iota(jnp.int32, (8, LANES), 0)
    columns = me * LANES + lane

    def table_step(i, carry):
        k, a = i // 16, lax.rem(i, 16) * 8 + sub
        at = tile(i)
        turns[0, at, :], turns[1, at, :] = cos_sin_quarter(
            ((8 * a + k) * columns).astype(F32) * (4.0 / TOTAL)
        )
        ticks[0, at, :], ticks[1, at, :] = cos_sin_quarter((a * k).astype(F32) * (4.0 / ROWS))
        return carry

    lax.fori_loop(0, 128, table_step, 0)

    def coefficient_step(i, carry):
        at = tile(i)
        block = coefficient_block(i * 8 + sub, columns, dispersion)
        for slot, value in block.items():
            coef[slot, 0, at, :] = value[0]
            coef[slot, 1, at, :] = value[1]
        return carry

    lax.fori_loop(0, 128, coefficient_step, 0)

    for load in loads[1:]:
        load.wait()
    both = w.at[:, pl.ds(0, (DEVICES - 1) * 8)]
    pltpu.make_async_copy(both, both, enter_sem.at[1]).wait()

    def pair(ref, at):
        return ref[0, at, :], ref[1, at, :]

    def stage(s, carry):
        def open_step(i, c):
            values = eight([pair(w, tile(16 * b + i)) for b in range(8)], 1.0)
            for k in range(8):
                value = times(values[k], pair(ticks, tile(16 * k + i))) if k else values[0]
                tmp[tile(i), k * LANES : (k + 1) * LANES] = value[0]
                tmp[tile(16 + i), k * LANES : (k + 1) * LANES] = value[1]
            return c

        lax.fori_loop(0, 16, open_step, 0)

        def out_step(g, c):
            for j in range(2):
                wide = pl.ds(pl.multiple_of(g * 512 + j * 256, 256), 256)
                real, imag = from_left(li, tmp[0:128, wide], tmp[128:256, wide])
                for h in range(2):
                    kk = 2 * j + h
                    at = pl.ds(pl.multiple_of((4 * g + kk) * 128, 128), 128)
                    cut = slice(h * LANES, (h + 1) * LANES)
                    value = times((real[:, cut], imag[:, cut]), pair(turns, at))
                    sb1[s, g, pl.ds(kk, 128, stride=8), :] = value[0]
                    sb1[s, g, pl.ds(4 + kk, 128, stride=8), :] = value[1]
            for other, there in partners():
                pltpu.make_async_remote_copy(
                    sb1.at[s, g, tile(other)], rb1.at[s, g, tile(me)],
                    s1.at[s, g], r1.at[s, g], device_id=there, device_id_type=MESH,
                ).start()
            rb1[s, g, tile(me), :] = sb1[s, g, tile(me), :]
            return c

        lax.fori_loop(0, 2, out_step, 0)

        def linear(body):
            lax.fori_loop(0, 128, lambda i, c: (body(tile(i)), c)[1], 0)

        def put(slot, at, value):
            lin[slot, 0, at, :] = value[0]
            lin[slot, 1, at, :] = value[1]

        @pl.when(s == 0)
        def _():
            def body(at):
                put(0, at, times(pair(coef.at[QUARTER], at), pair(w, at)))
                put(2, at, times(pair(coef.at[FULL], at), pair(w, at)))

            linear(body)

        @pl.when(s == 1)
        def _():
            def body(at):
                put(1, at, times(pair(coef.at[QUARTER], at), pair(w, at)))
                put(2, at, plus(pair(lin.at[2], at), times(pair(coef.at[FIRST], at), pair(nbuf.at[0], at))))

            linear(body)

        @pl.when(s >= 2)
        def _():
            def body(at):
                put(2, at, plus(pair(lin.at[2], at), times(pair(coef.at[SECOND], at), pair(nbuf.at[s - 1], at))))

            linear(body)

        def row_step(g, c):
            most = rb1.at[s, g, pl.ds(0, (DEVICES - 1) * 8)]
            pltpu.make_async_copy(most, most, r1.at[s, g]).wait()
            inner = tw[0], tw[1]
            for j in range(2):
                real = jnp.concatenate(
                    [rb1[s, g, pl.ds(2 * j + h, 128, stride=8), :] for h in range(2)], axis=1
                )
                imag = jnp.concatenate(
                    [rb1[s, g, pl.ds(4 + 2 * j + h, 128, stride=8), :] for h in range(2)], axis=1
                )
                real, imag = from_left(li, real, imag)
                halves = [
                    times((real[:, h * LANES : (h + 1) * LANES], imag[:, h * LANES : (h + 1) * LANES]), inner)
                    for h in range(2)
                ]
                real, imag = from_right(
                    ri,
                    jnp.concatenate([halves[0][0], halves[1][0]], axis=0),
                    jnp.concatenate([halves[0][1], halves[1][1]], axis=0),
                )
                size = -(real * real + imag * imag)
                real, imag = size * (real - twist * imag), size * (imag + twist * real)
                real, imag = from_right(rf, real, imag)
                halves = [
                    times_conj((real[h * 128 : (h + 1) * 128], imag[h * 128 : (h + 1) * 128]), inner)
                    for h in range(2)
                ]
                real, imag = from_left(
                    lf,
                    jnp.concatenate([halves[0][0], halves[1][0]], axis=1),
                    jnp.concatenate([halves[0][1], halves[1][1]], axis=1),
                )
                for h in range(2):
                    cut = slice(h * LANES, (h + 1) * LANES)
                    sb2[s, g, pl.ds(2 * j + h, 128, stride=8), :] = real[:, cut]
                    sb2[s, g, pl.ds(4 + 2 * j + h, 128, stride=8), :] = imag[:, cut]
            for other, there in partners():
                pltpu.make_async_remote_copy(
                    sb2.at[s, g, tile(other)], rb2.at[s, g, tile(me)],
                    s2.at[s, g], r2.at[s, g], device_id=there, device_id_type=MESH,
                ).start()
            rb2[s, g, tile(me), :] = sb2[s, g, tile(me), :]
            return c

        lax.fori_loop(0, 2, row_step, 0)

        def back_step(g, c):
            most = rb2.at[s, g, pl.ds(0, (DEVICES - 1) * 8)]
            pltpu.make_async_copy(most, most, r2.at[s, g]).wait()
            for j in range(2):
                halves = []
                for h in range(2):
                    kk = 2 * j + h
                    at = pl.ds(pl.multiple_of((4 * g + kk) * 128, 128), 128)
                    halves.append(
                        times_conj(
                            (
                                rb2[s, g, pl.ds(kk, 128, stride=8), :],
                                rb2[s, g, pl.ds(4 + kk, 128, stride=8), :],
                            ),
                            pair(turns, at),
                        )
                    )
                real, imag = from_left(
                    lf,
                    jnp.concatenate([halves[0][0], halves[1][0]], axis=1),
                    jnp.concatenate([halves[0][1], halves[1][1]], axis=1),
                )
                for h in range(2):
                    at = pl.ds(pl.multiple_of((4 * g + 2 * j + h) * 128, 128), 128)
                    cut = slice(h * LANES, (h + 1) * LANES)
                    mid[0, at, :] = real[:, cut]
                    mid[1, at, :] = imag[:, cut]
            return c

        lax.fori_loop(0, 2, back_step, 0)

        base = jnp.maximum(s - 1, 0)
        which = s // 3
        double = s == 2
        scale_new = jnp.where(double, 2.0, 1.0).astype(F32)
        scale_old = jnp.where(double, -1.0, 0.0).astype(F32)
        slot = HALF + which * (THIRD - HALF)

        def close_step(i, c):
            values = []
            for k in range(8):
                value = pair(mid, tile(16 * k + i))
                values.append(times_conj(value, pair(ticks, tile(16 * k + i))) if k else value)
            values = eight(values, -1.0)
            for b in range(8):
                at = tile(16 * b + i)
                new = values[b]
                nbuf[s, 0, at, :] = new[0]
                nbuf[s, 1, at, :] = new[1]
                old = pair(nbuf.at[0], at)
                mixed = (scale_new * new[0] + scale_old * old[0], scale_new * new[1] + scale_old * old[1])
                value = plus(pair(lin.at[base], at), times(pair(coef.at[slot], at), mixed))
                w[0, at, :] = value[0]
                w[1, at, :] = value[1]
            return c

        lax.fori_loop(0, 16, close_step, 0)
        return carry

    lax.fori_loop(0, 4, stage, 0)

    own = []
    for part in range(2):
        for other, there in partners():
            pltpu.make_async_remote_copy(
                w.at[part, tile(other)], o_hbm.at[part, :, band(me)],
                leave_sem.at[0], leave_sem.at[1], device_id=there, device_id_type=MESH,
            ).start()
        copy = pltpu.make_async_copy(w.at[part, tile(me)], o_hbm.at[part, :, band(me)], load_sem.at[part])
        copy.start()
        own.append(copy)

    pltpu.make_async_copy(both, both, enter_sem.at[0]).wait()

    def sent(s, carry):
        for g in range(2):
            for buffer, sem in ((sb1, s1), (sb2, s2)):
                most = buffer.at[s, g, pl.ds(0, (DEVICES - 1) * 8)]
                pltpu.make_async_copy(most, most, sem.at[s, g]).wait()
        return carry

    lax.fori_loop(0, 4, sent, 0)
    for copy in own:
        copy.wait()
    pltpu.make_async_copy(both, both, leave_sem.at[0]).wait()
    pltpu.make_async_copy(both, both, leave_sem.at[1]).wait()


def local(spectrum, parameters):
    hbm = pl.BlockSpec(memory_space=pl.ANY)
    field = (2, ROWS, LANES)
    return pl.pallas_call(
        kernel,
        name="etdrk4",
        out_shape=jax.ShapeDtypeStruct(spectrum.shape, F32),
        in_specs=[pl.BlockSpec(memory_space=pltpu.SMEM)] + [hbm] * 6,
        out_specs=hbm,
        scratch_shapes=[
            pltpu.VMEM(spectrum.shape, F32),
            pltpu.VMEM((256, 768), BF16),
            pltpu.VMEM((256, 768), BF16),
            pltpu.VMEM((768, 256), BF16),
            pltpu.VMEM((768, 256), BF16),
            pltpu.VMEM((2, 128, 128), F32),
            pltpu.VMEM(field, F32),
            pltpu.VMEM(field, F32),
            pltpu.VMEM((6,) + field, F32),
            pltpu.VMEM(field, F32),
            pltpu.VMEM((4,) + field, F32),
            pltpu.VMEM((3,) + field, F32),
            pltpu.VMEM((256, 1024), F32),
            pltpu.VMEM(field, F32),
        ]
        + [pltpu.VMEM((4, 2, 1024, LANES), F32)] * 4
        + [
            pltpu.SemaphoreType.DMA((6,)),
            pltpu.SemaphoreType.DMA((2,)),
            pltpu.SemaphoreType.DMA((2,)),
        ]
        + [pltpu.SemaphoreType.DMA((4, 2))] * 4,
        compiler_params=pltpu.CompilerParams(
            collective_id=0, has_side_effects=True, vmem_limit_bytes=60 * 1024 * 1024
        ),
    )(
        parameters,
        spectrum,
        jnp.asarray(left_table(1.0, 1.0)),
        jnp.asarray(left_table(-1.0, 1.0)),
        jnp.asarray(right_table(1.0, NORM)),
        jnp.asarray(right_table(-1.0, NORM)),
        jnp.asarray(inner_turns()),
    )


def solution(mesh):
    return jax.shard_map(
        local,
        mesh=mesh,
        in_specs=(P(None, ("gx", "gy"), None), P()),
        out_specs=P(None, ("gx", "gy"), None),
        check_vma=False,
    )
```

```python
import itertools
import math
import random

import jax
import jax.numpy as jnp
import numpy as np
from jax import lax
from jax.experimental import pallas as pl
from jax.experimental.pallas import tpu as pltpu
from jax.sharding import PartitionSpec as P

MESH = pl.DeviceIdType.MESH
F32 = jnp.float32
BF16 = jnp.bfloat16

time_step = 0.1
spacing = 0.25
DEVICES = 128
ROWS = 1024
COLS = 16384
TOTAL = ROWS * COLS
NORM = 1.0 / math.sqrt(TOTAL)
LANES = 128
PIECES = 4
STEP = 32

FULL, HALF, QUARTER, FIRST, SECOND, THIRD = 0, 2, 1, 3, 4, 5
WEIGHT, LAST = 0, 1


def offsets():
    every = [o for o in itertools.product(range(4), range(4), range(4), range(2)) if any(o)]
    random.Random(0).shuffle(every)
    every.sort(key=lambda o: -sum(min(v, 4 - v) for v in o[:3]))
    groups = {}
    for o in every:
        hop = next(((axis, o[axis]) for axis in (2, 1, 0) if o[axis]), None)
        groups.setdefault(hop, []).append(o)
    turns = itertools.zip_longest(*groups.values())
    return [o for turn in turns for o in turn if o is not None]


OTHERS = offsets()


def split_host(table):
    high = table.astype(np.float32).astype(jnp.bfloat16)
    low = (table - high.astype(np.float64)).astype(np.float32).astype(jnp.bfloat16)
    return high, low


def left_table(sign, scale):
    index = np.arange(128)
    angle = 2.0 * np.pi * (np.outer(index, index) % 128) / 128
    cosine, sine = np.cos(angle) * scale, sign * np.sin(angle) * scale
    high, low = split_host(np.block([[cosine, -sine], [sine, cosine]]))
    return np.concatenate([high, high, low], axis=1)


def right_table(sign, scale):
    index = np.arange(128)
    angle = 2.0 * np.pi * (np.outer(index, index) % 128) / 128
    cosine, sine = np.cos(angle) * scale, sign * np.sin(angle) * scale
    high, low = split_host(np.block([[cosine, sine], [-sine, cosine]]))
    return np.concatenate([high, high, low], axis=0)


def inner_turns():
    index = np.arange(128)
    angle = 2.0 * np.pi * np.outer(index, index) / COLS
    return np.stack([np.cos(angle), np.sin(angle)]).astype(np.float32)


def times(a, b):
    return a[0] * b[0] - a[1] * b[1], a[0] * b[1] + a[1] * b[0]


def times_conj(a, b):
    return a[0] * b[0] + a[1] * b[1], a[1] * b[0] - a[0] * b[1]


def plus(a, b):
    return a[0] + b[0], a[1] + b[1]


def minus(a, b):
    return a[0] - b[0], a[1] - b[1]


def turn(a, sign):
    return (-a[1], a[0]) if sign > 0 else (a[1], -a[0])


def four(x, sign):
    s02, d02 = plus(x[0], x[2]), minus(x[0], x[2])
    s13, d13 = plus(x[1], x[3]), turn(minus(x[1], x[3]), sign)
    return [plus(s02, s13), plus(d02, d13), minus(s02, s13), minus(d02, d13)]


def across(x, lower):
    return pltpu.roll(x, 64, 1) + jnp.where(lower, x, -x)


def swap(a, b, lower):
    return jnp.where(lower, a, pltpu.roll(b, 64, 1)), jnp.where(lower, pltpu.roll(a, 64, 1), b)


def eighth_turns(lower, sign):
    half = math.sqrt(0.5)
    return [
        (jnp.where(lower, 1.0, c), jnp.where(lower, 0.0, sign * v))
        for c, v in ((half, half), (0.0, 1.0), (-half, half))
    ]


def open_eight(x, lower):
    x = [(across(r, lower), across(i, lower)) for r, i in x]
    factors = eighth_turns(lower, 1.0)
    return four([x[0]] + [times(v, f) for v, f in zip(x[1:], factors)], 1.0)


def close_eight(x, lower):
    x = four(x, -1.0)
    factors = eighth_turns(lower, -1.0)
    x = [x[0]] + [times(v, f) for v, f in zip(x[1:], factors)]
    return [(across(r, lower), across(i, lower)) for r, i in x]


def cos_sin_quarter(quarters):
    whole = jnp.floor(quarters + 0.5)
    return cos_sin_near((quarters - whole) * (math.pi / 2), whole)


def cos_sin_near(x, whole):
    square = x * x
    sine = 1.0 / 362880.0
    for factor in (-1.0 / 5040.0, 1.0 / 120.0, -1.0 / 6.0, 1.0):
        sine = sine * square + factor
    sine = sine * x
    cosine = -1.0 / 3628800.0
    for factor in (1.0 / 40320.0, -1.0 / 720.0, 1.0 / 24.0, -0.5, 1.0):
        cosine = cosine * square + factor
    quadrant = whole.astype(jnp.int32) & 3
    swap = (quadrant & 1) == 1
    first = jnp.where(swap, sine, cosine)
    second = jnp.where(swap, cosine, sine)
    first = jnp.where((quadrant == 1) | (quadrant == 2), -first, first)
    second = jnp.where(quadrant >= 2, -second, second)
    return first, second


def cos_sin(x):
    whole = jnp.floor(x * (2.0 / math.pi) + 0.5)
    near = x - whole * 1.5703125
    near = near - whole * 4.837512969970703e-4
    near = near - whole * 7.549789948768648e-8
    return cos_sin_near(near, whole)


def series(z, order):
    real = jnp.full_like(z[0], 1.0 / math.factorial(14 + order))
    imag = jnp.zeros_like(z[0])
    for degree in range(13, -1, -1):
        real, imag = times((real, imag), z)
        real = real + 1.0 / math.factorial(degree + order)
    return real, imag


def over(z):
    scale = 1.0 / (z[0] * z[0] + z[1] * z[1])
    return z[0] * scale, -z[1] * scale


def pick(inside, a, b):
    return jnp.where(inside, a[0], b[0]), jnp.where(inside, a[1], b[1])


def coefficient_block(rows, columns, dispersion):
    mode = rows * COLS + columns
    signed = jnp.where(mode < TOTAL // 2, mode, mode - TOTAL).astype(F32)
    wavenum = signed * (2.0 * math.pi / (TOTAL * spacing))
    square = wavenum * wavenum
    z = time_step * (1.0 - square), -(time_step * dispersion * square)
    half = 0.5 * z[0], 0.5 * z[1]
    growth = jnp.exp(half[0])
    cosine, sine = cos_sin(half[1])
    decay_half = growth * cosine, growth * sine
    decay_full = times(decay_half, decay_half)

    inside = z[0] * z[0] + z[1] * z[1] < 1.0
    inverse = over((jnp.where(inside, 1.0, z[0]), jnp.where(inside, 0.0, z[1])))
    direct_one = times((decay_full[0] - 1.0, decay_full[1]), inverse)
    direct_two = times((direct_one[0] - 1.0, direct_one[1]), inverse)
    direct_three = times((direct_two[0] - 0.5, direct_two[1]), inverse)
    near_three = series(z, 3)
    near_two = times(near_three, z)
    near_two = near_two[0] + 0.5, near_two[1]
    near_one = times(near_two, z)
    near_one = near_one[0] + 1.0, near_one[1]
    one = pick(inside, near_one, direct_one)
    two = pick(inside, near_two, direct_two)
    three = pick(inside, near_three, direct_three)

    inside = half[0] * half[0] + half[1] * half[1] < 1.0
    inverse = over((jnp.where(inside, 1.0, half[0]), jnp.where(inside, 0.0, half[1])))
    direct = times((decay_half[0] - 1.0, decay_half[1]), inverse)
    half_one = pick(inside, series(half, 1), direct)

    return {
        FULL: decay_full,
        QUARTER: decay_half,
        HALF: tuple(0.5 * time_step * p for p in half_one),
        FIRST: tuple(time_step * (p - 3.0 * q + 4.0 * r) for p, q, r in zip(one, two, three)),
        SECOND: tuple(2.0 * time_step * (q - 2.0 * r) for q, r in zip(two, three)),
        THIRD: tuple(time_step * (4.0 * r - q) for q, r in zip(two, three)),
    }


def split(x):
    high = x.astype(BF16)
    return high, (x - high.astype(F32)).astype(BF16)


def from_left(table_ref, real, imag):
    high, low = split(jnp.concatenate([real, imag], axis=0))
    stacked = jnp.concatenate([high, low, high], axis=0)
    out = jnp.dot(table_ref[...], stacked, preferred_element_type=F32)
    return out[:128], out[128:]


def from_right(table_ref, real, imag):
    high, low = split(jnp.concatenate([real, imag], axis=1))
    stacked = jnp.concatenate([high, low, high], axis=1)
    out = jnp.dot(stacked, table_ref[...], preferred_element_type=F32)
    return out[:, :128], out[:, 128:]


def kernel(
    par, x_hbm, li_hbm, lf_hbm, ri_hbm, rf_hbm, tw_hbm,
    o_hbm,
    xin, packed, entered, li, lf, ri, rf, tw, turns, ticks, coef, w, nbuf, lin, tmp, mid, leaving,
    sb1, rb1, sb2, rb2,
    load_sem, enter_s, enter_r, leave_s, leave_r, s1, r1, s2, r2,
):
    gx, gy = lax.axis_index("gx"), lax.axis_index("gy")
    me = gx * 16 + gy
    z, y, x, core = me // 32, lax.rem(me // 8, 4), lax.rem(me // 2, 4), lax.rem(me, 2)
    zs = [lax.rem(z + i, 4) * 2 for i in range(4)]
    yh = [lax.rem(y + i, 4) // 2 for i in range(4)]
    yl = [lax.rem(lax.rem(y + i, 4), 2) * 8 for i in range(4)]
    xs = [lax.rem(x + i, 4) * 2 for i in range(4)]
    cs = [core, 1 - core]

    def partners():
        for oz, oy, ox, oc in OTHERS:
            tx = zs[oz] + yh[oy]
            ty = yl[oy] + xs[ox] + cs[oc]
            yield tx * 16 + ty, {"gx": tx, "gy": ty}

    def tile(index):
        return pl.ds(pl.multiple_of(index * 8, 8), 8)

    def half_tile(index, h):
        return pl.ds(pl.multiple_of(index * 8 + h * 4, 4), 4)

    def block(index):
        return pl.ds(pl.multiple_of(index * 128, 128), 128)

    def pair(ref, at):
        return ref[0, at, :], ref[1, at, :]

    def store(ref, at, value):
        ref[0, at, :] = value[0]
        ref[1, at, :] = value[1]

    def wait_for(ref, sem):
        pltpu.make_async_copy(ref, ref, sem).wait()

    def span(index, height):
        return pl.ds(pl.multiple_of(index, height), height)

    def loop(count, body, unroll=1):
        def step(i, carry):
            for j in range(unroll):
                body(i * unroll + j)
            return carry

        lax.fori_loop(0, count // unroll if unroll > 1 else count, step, 0)

    loads = [
        pltpu.make_async_copy(source, target, load_sem.at[i])
        for i, (source, target) in enumerate(
            [(x_hbm, xin), (li_hbm, li), (lf_hbm, lf), (ri_hbm, ri), (rf_hbm, rf), (tw_hbm, tw)]
        )
    ]
    loads[0].start()

    barrier = pltpu.get_barrier_semaphore()
    for _, there in partners():
        pl.semaphore_signal(barrier, 1, device_id=there, device_id_type=MESH)

    lane = lax.broadcasted_iota(jnp.int32, (8, LANES), 1)
    sub = lax.broadcasted_iota(jnp.int32, (8, LANES), 0)
    lower = lane < 64
    lower_tall = lax.broadcasted_iota(jnp.int32, (128, LANES), 1) < 64
    lower_step = lax.broadcasted_iota(jnp.int32, (STEP, LANES), 1) < 64
    upper_bit = lane // 64
    column = lax.rem(lane, 64)

    loads[0].wait()

    def pack(t):
        first, second = swap(xin[0, :, block(t)], xin[1, :, block(t)], lower)
        packed[0, tile(t), :] = first
        packed[1, tile(t), :] = second

    with jax.named_scope("pack"):
        loop(128, pack, 8)
    for load in loads[1:]:
        load.start()
    with jax.named_scope("greet"):
        pl.semaphore_wait(barrier, DEVICES - 1)

    def enter(h):
        for other, there in partners():
            pltpu.make_async_remote_copy(
                packed.at[h, tile(other)], entered.at[h, tile(me)],
                enter_s.at[h], enter_r.at[h], device_id=there, device_id_type=MESH,
            ).start()
        entered[h, tile(me), :] = packed[h, tile(me), :]

    with jax.named_scope("enter"):
        loop(2, enter)

    dispersion, twist = par[0], par[1]

    def turn_table(i):
        h, k, a = i // 64, lax.rem(i // 16, 4), lax.rem(i, 16) * 8 + sub
        number = (8 * a + 2 * k + upper_bit) * (me * LANES + 64 * h + column)
        store(turns.at[h], tile(lax.rem(i, 64)), cos_sin_quarter(number.astype(F32) * (4.0 / TOTAL)))

    with jax.named_scope("turn_table"):
        loop(128, turn_table, 4)

    def tick_table(i):
        number = (lax.rem(i, 16) * 8 + sub) * (2 * (i // 16) + upper_bit)
        store(ticks, tile(i), cos_sin_quarter(number.astype(F32) * (4.0 / ROWS)))

    with jax.named_scope("tick_table"):
        loop(64, tick_table, 4)


    def coefficient_table(h, i):
        at = tile(i)
        rows = i * 8 + sub + 512 * upper_bit
        for slot, value in coefficient_block(rows, me * LANES + 64 * h + column, dispersion).items():
            store(coef.at[slot, h], at, value)

    with jax.named_scope("coefs"):
        loop(64, lambda i: coefficient_table(0, i), 2)
    for load in loads[1:]:
        load.wait()

    def rows_of(digit, i):
        return span(digit * 128 + i * STEP, STEP)

    def open_rows(h, i, values):
        for k, value in enumerate(open_eight(values, lower_step)):
            value = times(value, pair(ticks, rows_of(k, i)))
            tmp[h, rows_of(0, i), k * LANES : (k + 1) * LANES] = value[0]
            tmp[h, rows_of(1, i), k * LANES : (k + 1) * LANES] = value[1]

    def closed_rows(h, i):
        values = [
            times_conj(pair(mid.at[h], rows_of(k, i)), pair(ticks, rows_of(k, i))) for k in range(4)
        ]
        return close_eight(values, lower_step)

    def back(s, g, h):
        with jax.named_scope("wait_back"):
            wait_for(rb2.at[s, g, pl.ds(0, (DEVICES - 1) * 4)], r2.at[s, g, h])
        values = []
        for k in range(2):
            value = (
                rb2[s, g, pl.ds(h * 4 + k, 128, stride=8), :],
                rb2[s, g, pl.ds(h * 4 + 2 + k, 128, stride=8), :],
            )
            values.append(times_conj(value, pair(turns.at[h], block(2 * g + k))))
        real, imag = from_left(
            lf,
            jnp.concatenate([values[0][0], values[1][0]], axis=1),
            jnp.concatenate([values[0][1], values[1][1]], axis=1),
        )
        for k in range(2):
            cut = slice(k * LANES, (k + 1) * LANES)
            store(mid.at[h], block(2 * g + k), (real[:, cut], imag[:, cut]))

    def stage(s, carry):
        def columns(h):
            @pl.when(s == 0)
            def _():
                with jax.named_scope("wait_enter"):
                    wait_for(entered.at[h, pl.ds(0, (DEVICES - 1) * 8)], enter_r.at[h])

                def body(i):
                    values = []
                    for b in range(4):
                        low = entered[h, rows_of(b, i), :]
                        high = entered[h, rows_of(b + 4, i), :]
                        values.append(swap(low, high, lower_step))
                    for b in range(4):
                        store(w.at[h], rows_of(b, i), values[b])
                    open_rows(h, i, values)

                with jax.named_scope("cols"):
                    loop(128 // STEP, body)

            @pl.when(s > 0)
            def _():
                with jax.named_scope("back1"):
                    back(s - 1, 1, h)

            @pl.when((s > 0) & (s < 4))
            def _():
                base = jnp.maximum(s - 2, 0)
                scale = jnp.where(s == 3, 2.0, 1.0).astype(F32)

                def body(i):
                    values = []
                    for b, new in enumerate(closed_rows(h, i)):
                        at = rows_of(b, i)
                        more = times(pair(coef.at[HALF, h], at), (scale * new[0], scale * new[1]))
                        values.append(plus(pair(lin.at[base, h], at), more))
                        store(nbuf.at[s - 1, h], at, new)
                        store(w.at[h], at, values[-1])
                    open_rows(h, i, values)

                with jax.named_scope("cols"):
                    loop(128 // STEP, body)

            @pl.when(s == 4)
            def _():
                def body(i):
                    for b, new in enumerate(closed_rows(h, i)):
                        at = rows_of(b, i)
                        value = plus(pair(lin.at[2, h], at), times(pair(coef.at[THIRD, h], at), new))
                        first, second = swap(value[0], value[1], lower_step)
                        leaving[h, at, :] = first
                        leaving[h, rows_of(b + 4, i), :] = second

                with jax.named_scope("cols"):
                    loop(128 // STEP, body)
                for other, there in partners():
                    pltpu.make_async_remote_copy(
                        leaving.at[h, tile(other)], o_hbm.at[h, tile(me)],
                        leave_s.at[h], leave_r.at[h], device_id=there, device_id_type=MESH,
                    ).start()
                pltpu.make_async_copy(leaving.at[h, tile(me)], o_hbm.at[h, tile(me)], load_sem.at[h]).start()

            @pl.when(s < 4)
            def _():
                def send(n):
                    half, g = lax.rem(h + n, 2), (n + 1) // 2
                    wide = pl.ds(pl.multiple_of(g * 256, 256), 256)
                    real, imag = from_left(li, tmp[half, 0:128, wide], tmp[half, 128:256, wide])
                    for k in range(2):
                        cut = slice(k * LANES, (k + 1) * LANES)
                        value = times((real[:, cut], imag[:, cut]), pair(turns.at[half], block(2 * g + k)))
                        sb1[s, g, pl.ds(half * 4 + k, 128, stride=8), :] = value[0]
                        sb1[s, g, pl.ds(half * 4 + 2 + k, 128, stride=8), :] = value[1]
                    for other, there in partners():
                        pltpu.make_async_remote_copy(
                            sb1.at[s, g, half_tile(other, half)], rb1.at[s, g, half_tile(me, half)],
                            s1.at[s, g], r1.at[s, g], device_id=there, device_id_type=MESH,
                        ).start()

                    @pl.when(half == 1)
                    def _():
                        rb1[s, g, tile(me), :] = sb1[s, g, tile(me), :]

                with jax.named_scope("sends1"):
                    loop(1 + 2 * h, send)

        loop(2, columns)

        def linear(body):
            def step(i):
                body(i // 16, span(lax.rem(i, 16) * 32, 32))

            with jax.named_scope("linear"):
                loop(32, step)

        def put(slot, h, at, value):
            store(lin.at[slot, h], at, value)

        @pl.when(s == 0)
        def _():
            with jax.named_scope("coefs1"):
                loop(64, lambda i: coefficient_table(1, i), 2)

            def body(h, at):
                value = pair(w.at[h], at)
                put(0, h, at, times(pair(coef.at[QUARTER, h], at), value))
                put(2, h, at, times(pair(coef.at[FULL, h], at), value))

            linear(body)

        @pl.when(s == 1)
        def _():
            def body(h, at):
                first = pair(nbuf.at[0, h], at)
                value = times(pair(coef.at[QUARTER, h], at), pair(w.at[h], at))
                less = times(pair(coef.at[HALF, h], at), first)
                more = plus(pair(lin.at[2, h], at), times(pair(coef.at[FIRST, h], at), first))
                put(1, h, at, minus(value, less))
                put(2, h, at, more)

            linear(body)

        @pl.when((s == 2) | (s == 3))
        def _():
            def body(h, at):
                more = times(pair(coef.at[SECOND, h], at), pair(nbuf.at[s - 1, h], at))
                put(2, h, at, plus(pair(lin.at[2, h], at), more))

            linear(body)

        def rows(g):
            with jax.named_scope("wait_rows"):
                wait_for(rb1.at[s, g, pl.ds(0, (DEVICES - 1) * 8)], r1.at[s, g])
            inner = tw[0], tw[1]

            def received(part, k):
                values = [
                    rb1[s, g, pl.ds(h * 4 + part * 2 + k, 128, stride=8), :] for h in range(2)
                ]
                return jnp.concatenate(swap(values[0], values[1], lower_tall), axis=1)

            for k in range(2):
                real, imag = from_left(li, received(0, k), received(1, k))
                parts = [
                    times((real[:, b * LANES : (b + 1) * LANES], imag[:, b * LANES : (b + 1) * LANES]), inner)
                    for b in range(2)
                ]
                real, imag = from_right(
                    ri,
                    jnp.concatenate([parts[0][0], parts[1][0]], axis=0),
                    jnp.concatenate([parts[0][1], parts[1][1]], axis=0),
                )
                size = -(real * real + imag * imag)
                real, imag = size * (real - twist * imag), size * (imag + twist * real)
                real, imag = from_right(rf, real, imag)
                parts = [
                    times_conj((real[b * 128 : (b + 1) * 128], imag[b * 128 : (b + 1) * 128]), inner)
                    for b in range(2)
                ]
                real, imag = from_left(
                    lf,
                    jnp.concatenate([parts[0][0], parts[1][0]], axis=1),
                    jnp.concatenate([parts[0][1], parts[1][1]], axis=1),
                )
                for part, value in enumerate((real, imag)):
                    for h, v in enumerate(swap(value[:, :LANES], value[:, LANES:], lower_tall)):
                        sb2[s, g, pl.ds(h * 4 + part * 2 + k, 128, stride=8), :] = v
            rb2[s, g, tile(me), :] = sb2[s, g, tile(me), :]

            def send(h):
                for other, there in partners():
                    pltpu.make_async_remote_copy(
                        sb2.at[s, g, half_tile(other, h)], rb2.at[s, g, half_tile(me, h)],
                        s2.at[s, g], r2.at[s, g, h], device_id=there, device_id_type=MESH,
                    ).start()

            with jax.named_scope("sends2"):
                loop(2, send)

        @pl.when(s < 4)
        def _():
            with jax.named_scope("rows"):
                loop(2, rows)
            with jax.named_scope("back0"):
                loop(2, lambda h: back(s, 0, h))

        return carry

    lax.fori_loop(0, 5, stage, 0)

    def sent(s):
        for g in range(2):
            for buffer, sem in ((sb1, s1), (sb2, s2)):
                wait_for(buffer.at[s, g, pl.ds(0, (DEVICES - 1) * 8)], sem.at[s, g])

    loop(4, sent)
    for h in range(2):
        most = packed.at[h, pl.ds(0, (DEVICES - 1) * 8)]
        wait_for(most, enter_s.at[h])
        wait_for(most, leave_s.at[h])
        pltpu.make_async_copy(leaving.at[h, tile(me)], o_hbm.at[h, tile(me)], load_sem.at[h]).wait()
        with jax.named_scope("wait_leave"):
            wait_for(most, leave_r.at[h])


def unpack_kernel(x_hbm, o_hbm, x_ref, o_ref, x_sem, o_sem):
    lower = lax.broadcasted_iota(jnp.int32, (8, LANES), 1) < 64
    tiles = DEVICES // PIECES
    into, out = [], []
    for i in range(PIECES):
        rows, lanes = pl.ds(i * tiles * 8, tiles * 8), pl.ds(i * tiles * LANES, tiles * LANES)
        into.append(pltpu.make_async_copy(x_hbm.at[:, rows], x_ref.at[:, rows], x_sem.at[i]))
        out.append(pltpu.make_async_copy(o_ref.at[:, :, lanes], o_hbm.at[:, :, lanes], o_sem.at[i]))
        into[-1].start()
    for i in range(PIECES):
        into[i].wait()
        for t in range(i * tiles, (i + 1) * tiles):
            at, lanes = slice(t * 8, t * 8 + 8), slice(t * LANES, t * LANES + LANES)
            o_ref[0, :, lanes], o_ref[1, :, lanes] = swap(x_ref[0, at, :], x_ref[1, at, :], lower)
        out[i].start()
    for copy in out:
        copy.wait()


def local(spectrum, parameters):
    hbm = pl.BlockSpec(memory_space=pl.ANY)
    field = (2, 2, ROWS // 2, LANES)
    whole = (2, ROWS, LANES)
    packed = pl.pallas_call(
        kernel,
        name="etdrk4",
        out_shape=jax.ShapeDtypeStruct(whole, F32),
        in_specs=[pl.BlockSpec(memory_space=pltpu.SMEM)] + [hbm] * 6,
        out_specs=hbm,
        scratch_shapes=[
            pltpu.VMEM(spectrum.shape, F32),
            pltpu.VMEM(whole, F32),
            pltpu.VMEM(whole, F32),
            pltpu.VMEM((256, 768), BF16),
            pltpu.VMEM((256, 768), BF16),
            pltpu.VMEM((768, 256), BF16),
            pltpu.VMEM((768, 256), BF16),
            pltpu.VMEM((2, 128, 128), F32),
            pltpu.VMEM(field, F32),
            pltpu.VMEM((2, ROWS // 2, LANES), F32),
            pltpu.VMEM((6,) + field, F32),
            pltpu.VMEM(field, F32),
            pltpu.VMEM((3,) + field, F32),
            pltpu.VMEM((3,) + field, F32),
            pltpu.VMEM((2, 256, 512), F32),
            pltpu.VMEM(field, F32),
            pltpu.VMEM(whole, F32),
        ]
        + [pltpu.VMEM((4, 2, ROWS, LANES), F32)] * 4
        + [pltpu.SemaphoreType.DMA((6,))]
        + [pltpu.SemaphoreType.DMA((2,))] * 4
        + [
            pltpu.SemaphoreType.DMA((4, 2)),
            pltpu.SemaphoreType.DMA((4, 2)),
            pltpu.SemaphoreType.DMA((4, 2)),
            pltpu.SemaphoreType.DMA((4, 2, 2)),
        ],
        compiler_params=pltpu.CompilerParams(
            collective_id=0, has_side_effects=True, vmem_limit_bytes=60 * 1024 * 1024
        ),
    )(
        parameters,
        spectrum,
        jnp.asarray(left_table(1.0, 1.0)),
        jnp.asarray(left_table(-1.0, 1.0)),
        jnp.asarray(right_table(1.0, NORM)),
        jnp.asarray(right_table(-1.0, NORM)),
        jnp.asarray(inner_turns()),
    )
    return pl.pallas_call(
        unpack_kernel,
        name="unpack",
        out_shape=jax.ShapeDtypeStruct(spectrum.shape, F32),
        in_specs=[hbm],
        out_specs=hbm,
        scratch_shapes=[
            pltpu.VMEM(whole, F32),
            pltpu.VMEM(spectrum.shape, F32),
            pltpu.SemaphoreType.DMA((PIECES,)),
            pltpu.SemaphoreType.DMA((PIECES,)),
        ],
        compiler_params=pltpu.CompilerParams(vmem_limit_bytes=60 * 1024 * 1024),
    )(packed)


def solution(mesh):
    return jax.shard_map(
        local,
        mesh=mesh,
        in_specs=(P(None, ("gx", "gy"), None), P()),
        out_specs=P(None, ("gx", "gy"), None),
        check_vma=False,
    )
```

```python
import itertools
import math
import random

import jax
import jax.numpy as jnp
import numpy as np
from jax import lax
from jax.experimental import pallas as pl
from jax.experimental.pallas import tpu as pltpu
from jax.sharding import PartitionSpec as P

MESH = pl.DeviceIdType.MESH
F32 = jnp.float32
BF16 = jnp.bfloat16

time_step = 0.1
spacing = 0.25
DEVICES = 128
ROWS = 1024
COLS = 16384
TOTAL = ROWS * COLS
NORM = 1.0 / math.sqrt(TOTAL)
LANES = 128
PACK = 16
PIECES = 4
STEP = 64

FULL, HALF, QUARTER, FIRST, SECOND, THIRD = 0, 2, 1, 3, 4, 5
WEIGHT, LAST = 0, 1


def offsets():
    every = [o for o in itertools.product(range(4), range(4), range(4), range(2)) if any(o)]
    random.Random(0).shuffle(every)
    every.sort(key=lambda o: -sum(min(v, 4 - v) for v in o[:3]))
    groups = {}
    for o in every:
        hop = next(((axis, o[axis]) for axis in (2, 1, 0) if o[axis]), None)
        groups.setdefault(hop, []).append(o)
    turns = itertools.zip_longest(*groups.values())
    return [o for turn in turns for o in turn if o is not None]


OTHERS = offsets()


def split_host(table):
    high = table.astype(np.float32).astype(jnp.bfloat16)
    low = (table - high.astype(np.float64)).astype(np.float32).astype(jnp.bfloat16)
    return high, low


def left_table(sign, scale):
    index = np.arange(128)
    angle = 2.0 * np.pi * (np.outer(index, index) % 128) / 128
    cosine, sine = np.cos(angle) * scale, sign * np.sin(angle) * scale
    high, low = split_host(np.block([[cosine, -sine], [sine, cosine]]))
    return np.concatenate([high, high, low], axis=1)


def right_table(sign, scale):
    index = np.arange(128)
    angle = 2.0 * np.pi * (np.outer(index, index) % 128) / 128
    cosine, sine = np.cos(angle) * scale, sign * np.sin(angle) * scale
    high, low = split_host(np.block([[cosine, sine], [-sine, cosine]]))
    return np.concatenate([high, high, low], axis=0)


def inner_turns():
    index = np.arange(128)
    angle = 2.0 * np.pi * np.outer(index, index) / COLS
    return np.stack([np.cos(angle), np.sin(angle)]).astype(np.float32)


def times(a, b):
    return a[0] * b[0] - a[1] * b[1], a[0] * b[1] + a[1] * b[0]


def times_conj(a, b):
    return a[0] * b[0] + a[1] * b[1], a[1] * b[0] - a[0] * b[1]


def plus(a, b):
    return a[0] + b[0], a[1] + b[1]


def minus(a, b):
    return a[0] - b[0], a[1] - b[1]


def turn(a, sign):
    return (-a[1], a[0]) if sign > 0 else (a[1], -a[0])


def four(x, sign):
    s02, d02 = plus(x[0], x[2]), minus(x[0], x[2])
    s13, d13 = plus(x[1], x[3]), turn(minus(x[1], x[3]), sign)
    return [plus(s02, s13), plus(d02, d13), minus(s02, s13), minus(d02, d13)]


def across(x, lower):
    return pltpu.roll(x, 64, 1) + jnp.where(lower, x, -x)


def swap(a, b, lower):
    return jnp.where(lower, a, pltpu.roll(b, 64, 1)), jnp.where(lower, pltpu.roll(a, 64, 1), b)


def eighth_turns(lower, sign):
    half = math.sqrt(0.5)
    return [
        (jnp.where(lower, 1.0, c), jnp.where(lower, 0.0, sign * v))
        for c, v in ((half, half), (0.0, 1.0), (-half, half))
    ]


def open_eight(x, lower):
    x = [(across(r, lower), across(i, lower)) for r, i in x]
    factors = eighth_turns(lower, 1.0)
    return four([x[0]] + [times(v, f) for v, f in zip(x[1:], factors)], 1.0)


def close_eight(x, lower):
    x = four(x, -1.0)
    factors = eighth_turns(lower, -1.0)
    x = [x[0]] + [times(v, f) for v, f in zip(x[1:], factors)]
    return [(across(r, lower), across(i, lower)) for r, i in x]


def cos_sin_quarter(quarters):
    whole = jnp.floor(quarters + 0.5)
    return cos_sin_near((quarters - whole) * (math.pi / 2), whole)


def cos_sin_near(x, whole):
    square = x * x
    sine = 1.0 / 362880.0
    for factor in (-1.0 / 5040.0, 1.0 / 120.0, -1.0 / 6.0, 1.0):
        sine = sine * square + factor
    sine = sine * x
    cosine = -1.0 / 3628800.0
    for factor in (1.0 / 40320.0, -1.0 / 720.0, 1.0 / 24.0, -0.5, 1.0):
        cosine = cosine * square + factor
    quadrant = whole.astype(jnp.int32) & 3
    swap = (quadrant & 1) == 1
    first = jnp.where(swap, sine, cosine)
    second = jnp.where(swap, cosine, sine)
    first = jnp.where((quadrant == 1) | (quadrant == 2), -first, first)
    second = jnp.where(quadrant >= 2, -second, second)
    return first, second


def cos_sin(x):
    whole = jnp.floor(x * (2.0 / math.pi) + 0.5)
    near = x - whole * 1.5703125
    near = near - whole * 4.837512969970703e-4
    near = near - whole * 7.549789948768648e-8
    return cos_sin_near(near, whole)


def series(z, order):
    real = jnp.full_like(z[0], 1.0 / math.factorial(14 + order))
    imag = jnp.zeros_like(z[0])
    for degree in range(13, -1, -1):
        real, imag = times((real, imag), z)
        real = real + 1.0 / math.factorial(degree + order)
    return real, imag


def over(z):
    scale = 1.0 / (z[0] * z[0] + z[1] * z[1])
    return z[0] * scale, -z[1] * scale


def pick(inside, a, b):
    return jnp.where(inside, a[0], b[0]), jnp.where(inside, a[1], b[1])


def coefficient_block(rows, columns, dispersion):
    mode = rows * COLS + columns
    signed = jnp.where(mode < TOTAL // 2, mode, mode - TOTAL).astype(F32)
    wavenum = signed * (2.0 * math.pi / (TOTAL * spacing))
    square = wavenum * wavenum
    z = time_step * (1.0 - square), -(time_step * dispersion * square)
    half = 0.5 * z[0], 0.5 * z[1]
    growth = jnp.exp(half[0])
    cosine, sine = cos_sin(half[1])
    decay_half = growth * cosine, growth * sine
    decay_full = times(decay_half, decay_half)

    inside = z[0] * z[0] + z[1] * z[1] < 1.0
    inverse = over((jnp.where(inside, 1.0, z[0]), jnp.where(inside, 0.0, z[1])))
    direct_one = times((decay_full[0] - 1.0, decay_full[1]), inverse)
    direct_two = times((direct_one[0] - 1.0, direct_one[1]), inverse)
    direct_three = times((direct_two[0] - 0.5, direct_two[1]), inverse)
    near_three = series(z, 3)
    near_two = times(near_three, z)
    near_two = near_two[0] + 0.5, near_two[1]
    near_one = times(near_two, z)
    near_one = near_one[0] + 1.0, near_one[1]
    one = pick(inside, near_one, direct_one)
    two = pick(inside, near_two, direct_two)
    three = pick(inside, near_three, direct_three)

    inside = half[0] * half[0] + half[1] * half[1] < 1.0
    inverse = over((jnp.where(inside, 1.0, half[0]), jnp.where(inside, 0.0, half[1])))
    direct = times((decay_half[0] - 1.0, decay_half[1]), inverse)
    half_one = pick(inside, series(half, 1), direct)

    return {
        FULL: decay_full,
        QUARTER: decay_half,
        HALF: tuple(0.5 * time_step * p for p in half_one),
        FIRST: tuple(time_step * (p - 3.0 * q + 4.0 * r) for p, q, r in zip(one, two, three)),
        SECOND: tuple(2.0 * time_step * (q - 2.0 * r) for q, r in zip(two, three)),
        THIRD: tuple(time_step * (4.0 * r - q) for q, r in zip(two, three)),
    }


def split(x):
    high = x.astype(BF16)
    return high, (x - high.astype(F32)).astype(BF16)


def from_left(table_ref, real, imag):
    high, low = split(jnp.concatenate([real, imag], axis=0))
    stacked = jnp.concatenate([high, low, high], axis=0)
    out = jnp.dot(table_ref[...], stacked, preferred_element_type=F32)
    return out[:128], out[128:]


def from_right(table_ref, real, imag):
    high, low = split(jnp.concatenate([real, imag], axis=1))
    stacked = jnp.concatenate([high, low, high], axis=1)
    out = jnp.dot(stacked, table_ref[...], preferred_element_type=F32)
    return out[:, :128], out[:, 128:]


def kernel(
    par, x_hbm, li_hbm, lf_hbm, ri_hbm, rf_hbm, tw_hbm,
    o_hbm,
    xin, packed, entered, li, lf, ri, rf, tw, turns, ticks, coef, w, nbuf, lin, tmp, mid, leaving,
    sb1, rb1, sb2, rb2,
    load_sem, enter_s, enter_r, leave_s, leave_r, s1, r1, s2, r2,
):
    gx, gy = lax.axis_index("gx"), lax.axis_index("gy")
    me = gx * 16 + gy
    z, y, x, core = me // 32, lax.rem(me // 8, 4), lax.rem(me // 2, 4), lax.rem(me, 2)
    zs = [lax.rem(z + i, 4) * 2 for i in range(4)]
    yh = [lax.rem(y + i, 4) // 2 for i in range(4)]
    yl = [lax.rem(lax.rem(y + i, 4), 2) * 8 for i in range(4)]
    xs = [lax.rem(x + i, 4) * 2 for i in range(4)]
    cs = [core, 1 - core]

    def partners():
        for oz, oy, ox, oc in OTHERS:
            tx = zs[oz] + yh[oy]
            ty = yl[oy] + xs[ox] + cs[oc]
            yield tx * 16 + ty, {"gx": tx, "gy": ty}

    def tile(index):
        return pl.ds(pl.multiple_of(index * 8, 8), 8)

    def half_tile(index, h):
        return pl.ds(pl.multiple_of(index * 8 + h * 4, 4), 4)

    def block(index):
        return pl.ds(pl.multiple_of(index * 128, 128), 128)

    def pair(ref, at):
        return ref[0, at, :], ref[1, at, :]

    def store(ref, at, value):
        ref[0, at, :] = value[0]
        ref[1, at, :] = value[1]

    def wait_for(ref, sem):
        pltpu.make_async_copy(ref, ref, sem).wait()

    def span(index, height):
        return pl.ds(pl.multiple_of(index, height), height)

    def loop(count, body, unroll=1):
        def step(i, carry):
            for j in range(unroll):
                body(i * unroll + j)
            return carry

        lax.fori_loop(0, count // unroll if unroll > 1 else count, step, 0)

    loads = []
    for i in range(PIECES):
        lanes = pl.ds(i * COLS // PIECES, COLS // PIECES)
        loads.append(pltpu.make_async_copy(x_hbm.at[:, :, lanes], xin.at[:, :, lanes], load_sem.at[i]))
        loads[i].start()
    for source, target in ((li_hbm, li), (lf_hbm, lf), (ri_hbm, ri), (rf_hbm, rf), (tw_hbm, tw)):
        loads.append(pltpu.make_async_copy(source, target, load_sem.at[len(loads)]))

    barrier = pltpu.get_barrier_semaphore()
    for _, there in partners():
        pl.semaphore_signal(barrier, 1, device_id=there, device_id_type=MESH)

    lane = lax.broadcasted_iota(jnp.int32, (8, LANES), 1)
    sub = lax.broadcasted_iota(jnp.int32, (8, LANES), 0)
    lower = lane < 64
    lower_tall = lax.broadcasted_iota(jnp.int32, (128, LANES), 1) < 64
    lower_step = lax.broadcasted_iota(jnp.int32, (STEP, LANES), 1) < 64
    upper_bit = lane // 64
    column = lax.rem(lane, 64)

    def pack(t):
        first, second = swap(xin[0, :, block(t)], xin[1, :, block(t)], lower)
        packed[0, tile(t), :] = first
        packed[1, tile(t), :] = second

    with jax.named_scope("pack"):
        for i in range(PIECES):
            loads[i].wait()
            first = i * 128 // PIECES
            loop(128 // PIECES, lambda t: pack(first + t), PACK)
    for load in loads[PIECES:]:
        load.start()
    with jax.named_scope("greet"):
        pl.semaphore_wait(barrier, DEVICES - 1)

    def enter(h):
        for other, there in partners():
            pltpu.make_async_remote_copy(
                packed.at[h, tile(other)], entered.at[h, tile(me)],
                enter_s.at[h], enter_r.at[h], device_id=there, device_id_type=MESH,
            ).start()
        entered[h, tile(me), :] = packed[h, tile(me), :]

    with jax.named_scope("enter"):
        loop(2, enter)

    dispersion, twist = par[0], par[1]

    def turn_table(i):
        h, k, a = i // 64, lax.rem(i // 16, 4), lax.rem(i, 16) * 8 + sub
        number = (8 * a + 2 * k + upper_bit) * (me * LANES + 64 * h + column)
        store(turns.at[h], tile(lax.rem(i, 64)), cos_sin_quarter(number.astype(F32) * (4.0 / TOTAL)))

    with jax.named_scope("turn_table"):
        loop(128, turn_table, 4)

    def tick_table(i):
        number = (lax.rem(i, 16) * 8 + sub) * (2 * (i // 16) + upper_bit)
        store(ticks, tile(i), cos_sin_quarter(number.astype(F32) * (4.0 / ROWS)))

    with jax.named_scope("tick_table"):
        loop(64, tick_table, 4)


    def coefficient_table(h, i):
        at = tile(i)
        rows = i * 8 + sub + 512 * upper_bit
        for slot, value in coefficient_block(rows, me * LANES + 64 * h + column, dispersion).items():
            store(coef.at[slot, h], at, value)

    with jax.named_scope("coefs"):
        loop(64, lambda i: coefficient_table(0, i), 2)
    for load in loads[PIECES:]:
        load.wait()

    def rows_of(digit, i):
        return span(digit * 128 + i * STEP, STEP)

    def open_rows(h, i, values):
        for k, value in enumerate(open_eight(values, lower_step)):
            value = times(value, pair(ticks, rows_of(k, i)))
            tmp[h, rows_of(0, i), k * LANES : (k + 1) * LANES] = value[0]
            tmp[h, rows_of(1, i), k * LANES : (k + 1) * LANES] = value[1]

    def closed_rows(h, i):
        values = [
            times_conj(pair(mid.at[h], rows_of(k, i)), pair(ticks, rows_of(k, i))) for k in range(4)
        ]
        return close_eight(values, lower_step)

    def back(s, g, h):
        with jax.named_scope("wait_back"):
            wait_for(rb2.at[s, g, pl.ds(0, (DEVICES - 1) * 4)], r2.at[s, g, h])
        values = []
        for k in range(2):
            value = (
                rb2[s, g, pl.ds(h * 4 + k, 128, stride=8), :],
                rb2[s, g, pl.ds(h * 4 + 2 + k, 128, stride=8), :],
            )
            values.append(times_conj(value, pair(turns.at[h], block(2 * g + k))))
        real, imag = from_left(
            lf,
            jnp.concatenate([values[0][0], values[1][0]], axis=1),
            jnp.concatenate([values[0][1], values[1][1]], axis=1),
        )
        for k in range(2):
            cut = slice(k * LANES, (k + 1) * LANES)
            store(mid.at[h], block(2 * g + k), (real[:, cut], imag[:, cut]))

    def stage(s, carry):
        def linear(body):
            def step(i):
                body(i // 16, span(lax.rem(i, 16) * 32, 32))

            with jax.named_scope("linear"):
                loop(32, step)

        def put(slot, h, at, value):
            store(lin.at[slot, h], at, value)

        def linear_parts():
            @pl.when(s == 1)
            def _():
                def body(h, at):
                    first = pair(nbuf.at[0, h], at)
                    value = times(pair(coef.at[QUARTER, h], at), pair(w.at[h], at))
                    less = times(pair(coef.at[HALF, h], at), first)
                    more = plus(pair(lin.at[2, h], at), times(pair(coef.at[FIRST, h], at), first))
                    put(1, h, at, minus(value, less))
                    put(2, h, at, more)

                linear(body)

            @pl.when((s == 2) | (s == 3))
            def _():
                def body(h, at):
                    more = times(pair(coef.at[SECOND, h], at), pair(nbuf.at[s - 1, h], at))
                    put(2, h, at, plus(pair(lin.at[2, h], at), more))

                linear(body)

        def columns(h):
            @pl.when(s == 0)
            def _():
                with jax.named_scope("wait_enter"):
                    wait_for(entered.at[h, pl.ds(0, (DEVICES - 1) * 8)], enter_r.at[h])

                def body(i):
                    values = []
                    for b in range(4):
                        low = entered[h, rows_of(b, i), :]
                        high = entered[h, rows_of(b + 4, i), :]
                        values.append(swap(low, high, lower_step))
                    for b in range(4):
                        store(w.at[h], rows_of(b, i), values[b])
                    open_rows(h, i, values)

                with jax.named_scope("cols"):
                    loop(128 // STEP, body)

            @pl.when(s > 0)
            def _():
                with jax.named_scope("back1"):
                    back(s - 1, 1, h)

            @pl.when((s > 0) & (s < 4))
            def _():
                base = jnp.maximum(s - 2, 0)
                scale = jnp.where(s == 3, 2.0, 1.0).astype(F32)

                def body(i):
                    values = []
                    for b, new in enumerate(closed_rows(h, i)):
                        at = rows_of(b, i)
                        more = times(pair(coef.at[HALF, h], at), (scale * new[0], scale * new[1]))
                        values.append(plus(pair(lin.at[base, h], at), more))
                        store(nbuf.at[s - 1, h], at, new)
                        store(w.at[h], at, values[-1])
                    open_rows(h, i, values)

                with jax.named_scope("cols"):
                    loop(128 // STEP, body)

            @pl.when(s == 4)
            def _():
                def body(i):
                    for b, new in enumerate(closed_rows(h, i)):
                        at = rows_of(b, i)
                        value = plus(pair(lin.at[2, h], at), times(pair(coef.at[THIRD, h], at), new))
                        first, second = swap(value[0], value[1], lower_step)
                        leaving[h, at, :] = first
                        leaving[h, rows_of(b + 4, i), :] = second

                with jax.named_scope("cols"):
                    loop(128 // STEP, body)
                for other, there in partners():
                    pltpu.make_async_remote_copy(
                        leaving.at[h, tile(other)], o_hbm.at[h, tile(me)],
                        leave_s.at[h], leave_r.at[h], device_id=there, device_id_type=MESH,
                    ).start()
                pltpu.make_async_copy(leaving.at[h, tile(me)], o_hbm.at[h, tile(me)], load_sem.at[h]).start()

            @pl.when(s < 4)
            def _():
                def send(n):
                    half, g = lax.rem(h + n, 2), (n + 1) // 2

                    @pl.when(n == 1)
                    def _():
                        linear_parts()

                    wide = pl.ds(pl.multiple_of(g * 256, 256), 256)
                    real, imag = from_left(li, tmp[half, 0:128, wide], tmp[half, 128:256, wide])
                    for k in range(2):
                        cut = slice(k * LANES, (k + 1) * LANES)
                        value = times((real[:, cut], imag[:, cut]), pair(turns.at[half], block(2 * g + k)))
                        sb1[s, g, pl.ds(half * 4 + k, 128, stride=8), :] = value[0]
                        sb1[s, g, pl.ds(half * 4 + 2 + k, 128, stride=8), :] = value[1]
                    for other, there in partners():
                        pltpu.make_async_remote_copy(
                            sb1.at[s, g, half_tile(other, half)], rb1.at[s, g, half_tile(me, half)],
                            s1.at[s, g], r1.at[s, g], device_id=there, device_id_type=MESH,
                        ).start()

                    @pl.when(half == 1)
                    def _():
                        rb1[s, g, tile(me), :] = sb1[s, g, tile(me), :]

                with jax.named_scope("sends1"):
                    loop(1 + 2 * h, send)

        loop(2, columns)

        @pl.when(s == 0)
        def _():
            with jax.named_scope("coefs1"):
                loop(64, lambda i: coefficient_table(1, i), 2)

            def body(h, at):
                value = pair(w.at[h], at)
                put(0, h, at, times(pair(coef.at[QUARTER, h], at), value))
                put(2, h, at, times(pair(coef.at[FULL, h], at), value))

            linear(body)

        def rows(g):
            with jax.named_scope("wait_rows"):
                wait_for(rb1.at[s, g, pl.ds(0, (DEVICES - 1) * 8)], r1.at[s, g])
            inner = tw[0], tw[1]

            def received(part, k):
                values = [
                    rb1[s, g, pl.ds(h * 4 + part * 2 + k, 128, stride=8), :] for h in range(2)
                ]
                return jnp.concatenate(swap(values[0], values[1], lower_tall), axis=1)

            for k in range(2):
                real, imag = from_left(li, received(0, k), received(1, k))
                parts = [
                    times((real[:, b * LANES : (b + 1) * LANES], imag[:, b * LANES : (b + 1) * LANES]), inner)
                    for b in range(2)
                ]
                real, imag = from_right(
                    ri,
                    jnp.concatenate([parts[0][0], parts[1][0]], axis=0),
                    jnp.concatenate([parts[0][1], parts[1][1]], axis=0),
                )
                size = -(real * real + imag * imag)
                real, imag = size * (real - twist * imag), size * (imag + twist * real)
                real, imag = from_right(rf, real, imag)
                parts = [
                    times_conj((real[b * 128 : (b + 1) * 128], imag[b * 128 : (b + 1) * 128]), inner)
                    for b in range(2)
                ]
                real, imag = from_left(
                    lf,
                    jnp.concatenate([parts[0][0], parts[1][0]], axis=1),
                    jnp.concatenate([parts[0][1], parts[1][1]], axis=1),
                )
                for part, value in enumerate((real, imag)):
                    for h, v in enumerate(swap(value[:, :LANES], value[:, LANES:], lower_tall)):
                        sb2[s, g, pl.ds(h * 4 + part * 2 + k, 128, stride=8), :] = v
            rb2[s, g, tile(me), :] = sb2[s, g, tile(me), :]

            def send(h):
                for other, there in partners():
                    pltpu.make_async_remote_copy(
                        sb2.at[s, g, half_tile(other, h)], rb2.at[s, g, half_tile(me, h)],
                        s2.at[s, g], r2.at[s, g, h], device_id=there, device_id_type=MESH,
                    ).start()

            with jax.named_scope("sends2"):
                loop(2, send)

        @pl.when(s < 4)
        def _():
            with jax.named_scope("rows"):
                loop(2, rows)
            with jax.named_scope("back0"):
                loop(2, lambda h: back(s, 0, h))

        return carry

    lax.fori_loop(0, 5, stage, 0)

    def sent(s):
        for g in range(2):
            for buffer, sem in ((sb1, s1), (sb2, s2)):
                wait_for(buffer.at[s, g, pl.ds(0, (DEVICES - 1) * 8)], sem.at[s, g])

    loop(4, sent)
    for h in range(2):
        most = packed.at[h, pl.ds(0, (DEVICES - 1) * 8)]
        wait_for(most, enter_s.at[h])
        wait_for(most, leave_s.at[h])
        pltpu.make_async_copy(leaving.at[h, tile(me)], o_hbm.at[h, tile(me)], load_sem.at[h]).wait()
        with jax.named_scope("wait_leave"):
            wait_for(most, leave_r.at[h])


def unpack_kernel(x_hbm, o_hbm, x_ref, o_ref, x_sem, o_sem):
    lower = lax.broadcasted_iota(jnp.int32, (8, LANES), 1) < 64
    tiles = DEVICES // PIECES
    into, out = [], []
    for i in range(PIECES):
        rows, lanes = pl.ds(i * tiles * 8, tiles * 8), pl.ds(i * tiles * LANES, tiles * LANES)
        into.append(pltpu.make_async_copy(x_hbm.at[:, rows], x_ref.at[:, rows], x_sem.at[i]))
        out.append(pltpu.make_async_copy(o_ref.at[:, :, lanes], o_hbm.at[:, :, lanes], o_sem.at[i]))
        into[-1].start()
    for i in range(PIECES):
        into[i].wait()
        for t in range(i * tiles, (i + 1) * tiles):
            at, lanes = slice(t * 8, t * 8 + 8), slice(t * LANES, t * LANES + LANES)
            o_ref[0, :, lanes], o_ref[1, :, lanes] = swap(x_ref[0, at, :], x_ref[1, at, :], lower)
        out[i].start()
    for copy in out:
        copy.wait()


def local(spectrum, parameters):
    hbm = pl.BlockSpec(memory_space=pl.ANY)
    field = (2, 2, ROWS // 2, LANES)
    whole = (2, ROWS, LANES)
    packed = pl.pallas_call(
        kernel,
        name="etdrk4",
        out_shape=jax.ShapeDtypeStruct(whole, F32),
        in_specs=[pl.BlockSpec(memory_space=pltpu.SMEM)] + [hbm] * 6,
        out_specs=hbm,
        scratch_shapes=[
            pltpu.VMEM(spectrum.shape, F32),
            pltpu.VMEM(whole, F32),
            pltpu.VMEM(whole, F32),
            pltpu.VMEM((256, 768), BF16),
            pltpu.VMEM((256, 768), BF16),
            pltpu.VMEM((768, 256), BF16),
            pltpu.VMEM((768, 256), BF16),
            pltpu.VMEM((2, 128, 128), F32),
            pltpu.VMEM(field, F32),
            pltpu.VMEM((2, ROWS // 2, LANES), F32),
            pltpu.VMEM((6,) + field, F32),
            pltpu.VMEM(field, F32),
            pltpu.VMEM((3,) + field, F32),
            pltpu.VMEM((3,) + field, F32),
            pltpu.VMEM((2, 256, 512), F32),
            pltpu.VMEM(field, F32),
            pltpu.VMEM(whole, F32),
        ]
        + [pltpu.VMEM((4, 2, ROWS, LANES), F32)] * 4
        + [pltpu.SemaphoreType.DMA((PIECES + 5,))]
        + [pltpu.SemaphoreType.DMA((2,))] * 4
        + [
            pltpu.SemaphoreType.DMA((4, 2)),
            pltpu.SemaphoreType.DMA((4, 2)),
            pltpu.SemaphoreType.DMA((4, 2)),
            pltpu.SemaphoreType.DMA((4, 2, 2)),
        ],
        compiler_params=pltpu.CompilerParams(
            collective_id=0, has_side_effects=True, vmem_limit_bytes=60 * 1024 * 1024
        ),
    )(
        parameters,
        spectrum,
        jnp.asarray(left_table(1.0, 1.0)),
        jnp.asarray(left_table(-1.0, 1.0)),
        jnp.asarray(right_table(1.0, NORM)),
        jnp.asarray(right_table(-1.0, NORM)),
        jnp.asarray(inner_turns()),
    )
    return pl.pallas_call(
        unpack_kernel,
        name="unpack",
        out_shape=jax.ShapeDtypeStruct(spectrum.shape, F32),
        in_specs=[hbm],
        out_specs=hbm,
        scratch_shapes=[
            pltpu.VMEM(whole, F32),
            pltpu.VMEM(spectrum.shape, F32),
            pltpu.SemaphoreType.DMA((PIECES,)),
            pltpu.SemaphoreType.DMA((PIECES,)),
        ],
        compiler_params=pltpu.CompilerParams(vmem_limit_bytes=60 * 1024 * 1024),
    )(packed)


def solution(mesh):
    return jax.shard_map(
        local,
        mesh=mesh,
        in_specs=(P(None, ("gx", "gy"), None), P()),
        out_specs=P(None, ("gx", "gy"), None),
        check_vma=False,
    )
```

```python
import itertools
import math

import jax
import jax.numpy as jnp
import numpy as np
from jax import lax
from jax.experimental import pallas as pl
from jax.experimental.pallas import tpu as pltpu
from jax.sharding import PartitionSpec as P

MESH = pl.DeviceIdType.MESH
F32 = jnp.float32
BF16 = jnp.bfloat16

time_step = 0.1
spacing = 0.25
DEVICES = 128
ROWS = 1024
COLS = 16384
TOTAL = ROWS * COLS
NORM = 1.0 / math.sqrt(TOTAL)
LANES = 128
PACK = 16
PIECES = 4
STEP = 64

FULL, HALF, QUARTER, FIRST, SECOND, THIRD = 0, 2, 1, 3, 4, 5
WEIGHT, LAST = 0, 1


def offsets():
    every = [o for o in itertools.product(range(4), range(4), range(4), range(2)) if any(o)]
    every.sort(key=lambda o: -sum(min(v, 4 - v) for v in o[:3]))
    groups = {}
    for o in every:
        hop = next(((axis, o[axis]) for axis in (2, 1, 0) if o[axis]), None)
        groups.setdefault(hop, []).append(o)
    turns = itertools.zip_longest(*groups.values())
    return [o for turn in turns for o in turn if o is not None]


OTHERS = offsets()


def split_host(table):
    high = table.astype(np.float32).astype(jnp.bfloat16)
    low = (table - high.astype(np.float64)).astype(np.float32).astype(jnp.bfloat16)
    return high, low


def left_table(sign, scale):
    index = np.arange(128)
    angle = 2.0 * np.pi * (np.outer(index, index) % 128) / 128
    cosine, sine = np.cos(angle) * scale, sign * np.sin(angle) * scale
    high, low = split_host(np.block([[cosine, -sine], [sine, cosine]]))
    return np.concatenate([high, high, low], axis=1)


def right_table(sign, scale):
    index = np.arange(128)
    angle = 2.0 * np.pi * (np.outer(index, index) % 128) / 128
    cosine, sine = np.cos(angle) * scale, sign * np.sin(angle) * scale
    high, low = split_host(np.block([[cosine, sine], [-sine, cosine]]))
    return np.concatenate([high, high, low], axis=0)


def inner_turns():
    index = np.arange(128)
    angle = 2.0 * np.pi * np.outer(index, index) / COLS
    return np.stack([np.cos(angle), np.sin(angle)]).astype(np.float32)


def times(a, b):
    return a[0] * b[0] - a[1] * b[1], a[0] * b[1] + a[1] * b[0]


def times_conj(a, b):
    return a[0] * b[0] + a[1] * b[1], a[1] * b[0] - a[0] * b[1]


def plus(a, b):
    return a[0] + b[0], a[1] + b[1]


def minus(a, b):
    return a[0] - b[0], a[1] - b[1]


def turn(a, sign):
    return (-a[1], a[0]) if sign > 0 else (a[1], -a[0])


def four(x, sign):
    s02, d02 = plus(x[0], x[2]), minus(x[0], x[2])
    s13, d13 = plus(x[1], x[3]), turn(minus(x[1], x[3]), sign)
    return [plus(s02, s13), plus(d02, d13), minus(s02, s13), minus(d02, d13)]


def across(x, lower):
    return pltpu.roll(x, 64, 1) + jnp.where(lower, x, -x)


def swap(a, b, lower):
    return jnp.where(lower, a, pltpu.roll(b, 64, 1)), jnp.where(lower, pltpu.roll(a, 64, 1), b)


def eighth_turns(lower, sign):
    half = math.sqrt(0.5)
    return [
        (jnp.where(lower, 1.0, c), jnp.where(lower, 0.0, sign * v))
        for c, v in ((half, half), (0.0, 1.0), (-half, half))
    ]


def open_eight(x, lower):
    x = [(across(r, lower), across(i, lower)) for r, i in x]
    factors = eighth_turns(lower, 1.0)
    return four([x[0]] + [times(v, f) for v, f in zip(x[1:], factors)], 1.0)


def close_eight(x, lower):
    x = four(x, -1.0)
    factors = eighth_turns(lower, -1.0)
    x = [x[0]] + [times(v, f) for v, f in zip(x[1:], factors)]
    return [(across(r, lower), across(i, lower)) for r, i in x]


def cos_sin_quarter(quarters):
    whole = jnp.floor(quarters + 0.5)
    return cos_sin_near((quarters - whole) * (math.pi / 2), whole)


def cos_sin_near(x, whole):
    square = x * x
    sine = 1.0 / 362880.0
    for factor in (-1.0 / 5040.0, 1.0 / 120.0, -1.0 / 6.0, 1.0):
        sine = sine * square + factor
    sine = sine * x
    cosine = -1.0 / 3628800.0
    for factor in (1.0 / 40320.0, -1.0 / 720.0, 1.0 / 24.0, -0.5, 1.0):
        cosine = cosine * square + factor
    quadrant = whole.astype(jnp.int32) & 3
    swap = (quadrant & 1) == 1
    first = jnp.where(swap, sine, cosine)
    second = jnp.where(swap, cosine, sine)
    first = jnp.where((quadrant == 1) | (quadrant == 2), -first, first)
    second = jnp.where(quadrant >= 2, -second, second)
    return first, second


def cos_sin(x):
    whole = jnp.floor(x * (2.0 / math.pi) + 0.5)
    near = x - whole * 1.5703125
    near = near - whole * 4.837512969970703e-4
    near = near - whole * 7.549789948768648e-8
    return cos_sin_near(near, whole)


def series(z, order):
    real = jnp.full_like(z[0], 1.0 / math.factorial(14 + order))
    imag = jnp.zeros_like(z[0])
    for degree in range(13, -1, -1):
        real, imag = times((real, imag), z)
        real = real + 1.0 / math.factorial(degree + order)
    return real, imag


def over(z):
    scale = 1.0 / (z[0] * z[0] + z[1] * z[1])
    return z[0] * scale, -z[1] * scale


def pick(inside, a, b):
    return jnp.where(inside, a[0], b[0]), jnp.where(inside, a[1], b[1])


def coefficient_block(rows, columns, dispersion):
    mode = rows * COLS + columns
    signed = jnp.where(mode < TOTAL // 2, mode, mode - TOTAL).astype(F32)
    wavenum = signed * (2.0 * math.pi / (TOTAL * spacing))
    square = wavenum * wavenum
    z = time_step * (1.0 - square), -(time_step * dispersion * square)
    half = 0.5 * z[0], 0.5 * z[1]
    growth = jnp.exp(half[0])
    cosine, sine = cos_sin(half[1])
    decay_half = growth * cosine, growth * sine
    decay_full = times(decay_half, decay_half)

    inside = z[0] * z[0] + z[1] * z[1] < 1.0
    inverse = over((jnp.where(inside, 1.0, z[0]), jnp.where(inside, 0.0, z[1])))
    direct_one = times((decay_full[0] - 1.0, decay_full[1]), inverse)
    direct_two = times((direct_one[0] - 1.0, direct_one[1]), inverse)
    direct_three = times((direct_two[0] - 0.5, direct_two[1]), inverse)
    near_three = series(z, 3)
    near_two = times(near_three, z)
    near_two = near_two[0] + 0.5, near_two[1]
    near_one = times(near_two, z)
    near_one = near_one[0] + 1.0, near_one[1]
    one = pick(inside, near_one, direct_one)
    two = pick(inside, near_two, direct_two)
    three = pick(inside, near_three, direct_three)

    inside = half[0] * half[0] + half[1] * half[1] < 1.0
    inverse = over((jnp.where(inside, 1.0, half[0]), jnp.where(inside, 0.0, half[1])))
    direct = times((decay_half[0] - 1.0, decay_half[1]), inverse)
    half_one = pick(inside, series(half, 1), direct)

    return {
        FULL: decay_full,
        QUARTER: decay_half,
        HALF: tuple(0.5 * time_step * p for p in half_one),
        FIRST: tuple(time_step * (p - 3.0 * q + 4.0 * r) for p, q, r in zip(one, two, three)),
        SECOND: tuple(2.0 * time_step * (q - 2.0 * r) for q, r in zip(two, three)),
        THIRD: tuple(time_step * (4.0 * r - q) for q, r in zip(two, three)),
    }


def split(x):
    high = x.astype(BF16)
    return high, (x - high.astype(F32)).astype(BF16)


def from_left(table_ref, real, imag):
    high, low = split(jnp.concatenate([real, imag], axis=0))
    stacked = jnp.concatenate([high, low, high], axis=0)
    out = jnp.dot(table_ref[...], stacked, preferred_element_type=F32)
    return out[:128], out[128:]


def from_right(table_ref, real, imag):
    high, low = split(jnp.concatenate([real, imag], axis=1))
    stacked = jnp.concatenate([high, low, high], axis=1)
    out = jnp.dot(stacked, table_ref[...], preferred_element_type=F32)
    return out[:, :128], out[:, 128:]


def kernel(
    par, x_hbm, li_hbm, lf_hbm, ri_hbm, rf_hbm, tw_hbm,
    o_hbm,
    xin, packed, entered, li, lf, ri, rf, tw, turns, ticks, coef, w, nbuf, lin, tmp, mid, leaving,
    sb1, rb1, sb2, rb2,
    load_sem, enter_s, enter_r, leave_s, leave_r, s1, r1, s2, r2,
):
    gx, gy = lax.axis_index("gx"), lax.axis_index("gy")
    me = gx * 16 + gy
    z, y, x, core = me // 32, lax.rem(me // 8, 4), lax.rem(me // 2, 4), lax.rem(me, 2)
    zs = [lax.rem(z + i, 4) * 2 for i in range(4)]
    yh = [lax.rem(y + i, 4) // 2 for i in range(4)]
    yl = [lax.rem(lax.rem(y + i, 4), 2) * 8 for i in range(4)]
    xs = [lax.rem(x + i, 4) * 2 for i in range(4)]
    cs = [core, 1 - core]

    def partners():
        for oz, oy, ox, oc in OTHERS:
            tx = zs[oz] + yh[oy]
            ty = yl[oy] + xs[ox] + cs[oc]
            yield tx * 16 + ty, {"gx": tx, "gy": ty}

    def tile(index):
        return pl.ds(pl.multiple_of(index * 8, 8), 8)

    def half_tile(index, h):
        return pl.ds(pl.multiple_of(index * 8 + h * 4, 4), 4)

    def block(index):
        return pl.ds(pl.multiple_of(index * 128, 128), 128)

    def pair(ref, at):
        return ref[0, at, :], ref[1, at, :]

    def store(ref, at, value):
        ref[0, at, :] = value[0]
        ref[1, at, :] = value[1]

    def wait_for(ref, sem):
        pltpu.make_async_copy(ref, ref, sem).wait()

    def span(index, height):
        return pl.ds(pl.multiple_of(index, height), height)

    def loop(count, body, unroll=1):
        def step(i, carry):
            for j in range(unroll):
                body(i * unroll + j)
            return carry

        lax.fori_loop(0, count // unroll if unroll > 1 else count, step, 0)

    loads = []
    for i in range(PIECES):
        lanes = pl.ds(i * COLS // PIECES, COLS // PIECES)
        loads.append(pltpu.make_async_copy(x_hbm.at[:, :, lanes], xin.at[:, :, lanes], load_sem.at[i]))
        loads[i].start()
    for source, target in ((li_hbm, li), (lf_hbm, lf), (ri_hbm, ri), (rf_hbm, rf), (tw_hbm, tw)):
        loads.append(pltpu.make_async_copy(source, target, load_sem.at[len(loads)]))

    barrier = pltpu.get_barrier_semaphore()
    for _, there in partners():
        pl.semaphore_signal(barrier, 1, device_id=there, device_id_type=MESH)

    lane = lax.broadcasted_iota(jnp.int32, (8, LANES), 1)
    sub = lax.broadcasted_iota(jnp.int32, (8, LANES), 0)
    lower = lane < 64
    lower_tall = lax.broadcasted_iota(jnp.int32, (128, LANES), 1) < 64
    lower_step = lax.broadcasted_iota(jnp.int32, (STEP, LANES), 1) < 64
    upper_bit = lane // 64
    column = lax.rem(lane, 64)

    def pack(t):
        first, second = swap(xin[0, :, block(t)], xin[1, :, block(t)], lower)
        packed[0, tile(t), :] = first
        packed[1, tile(t), :] = second

    with jax.named_scope("pack"):
        for i in range(PIECES):
            loads[i].wait()
            first = i * 128 // PIECES
            loop(128 // PIECES, lambda t: pack(first + t), PACK)
    for load in loads[PIECES:]:
        load.start()
    with jax.named_scope("greet"):
        pl.semaphore_wait(barrier, DEVICES - 1)

    def enter(h):
        for other, there in partners():
            pltpu.make_async_remote_copy(
                packed.at[h, tile(other)], entered.at[h, tile(me)],
                enter_s.at[h], enter_r.at[h], device_id=there, device_id_type=MESH,
            ).start()
        entered[h, tile(me), :] = packed[h, tile(me), :]

    with jax.named_scope("enter"):
        loop(2, enter)

    dispersion, twist = par[0], par[1]

    def turn_table(i):
        h, k, a = i // 64, lax.rem(i // 16, 4), lax.rem(i, 16) * 8 + sub
        number = (8 * a + 2 * k + upper_bit) * (me * LANES + 64 * h + column)
        store(turns.at[h], tile(lax.rem(i, 64)), cos_sin_quarter(number.astype(F32) * (4.0 / TOTAL)))

    with jax.named_scope("turn_table"):
        loop(128, turn_table, 4)

    def tick_table(i):
        number = (lax.rem(i, 16) * 8 + sub) * (2 * (i // 16) + upper_bit)
        store(ticks, tile(i), cos_sin_quarter(number.astype(F32) * (4.0 / ROWS)))

    with jax.named_scope("tick_table"):
        loop(64, tick_table, 4)


    def coefficient_table(h, i):
        at = tile(i)
        rows = i * 8 + sub + 512 * upper_bit
        for slot, value in coefficient_block(rows, me * LANES + 64 * h + column, dispersion).items():
            store(coef.at[slot, h], at, value)

    with jax.named_scope("coefs"):
        loop(64, lambda i: coefficient_table(0, i), 2)
    for load in loads[PIECES:]:
        load.wait()

    def rows_of(digit, i):
        return span(digit * 128 + i * STEP, STEP)

    def open_rows(h, i, values):
        for k, value in enumerate(open_eight(values, lower_step)):
            value = times(value, pair(ticks, rows_of(k, i)))
            tmp[h, rows_of(0, i), k * LANES : (k + 1) * LANES] = value[0]
            tmp[h, rows_of(1, i), k * LANES : (k + 1) * LANES] = value[1]

    def closed_rows(h, i):
        values = [
            times_conj(pair(mid.at[h], rows_of(k, i)), pair(ticks, rows_of(k, i))) for k in range(4)
        ]
        return close_eight(values, lower_step)

    def back(s, g, h):
        with jax.named_scope("wait_back"):
            wait_for(rb2.at[s, g, pl.ds(0, (DEVICES - 1) * 4)], r2.at[s, g, h])
        values = []
        for k in range(2):
            value = (
                rb2[s, g, pl.ds(h * 4 + k, 128, stride=8), :],
                rb2[s, g, pl.ds(h * 4 + 2 + k, 128, stride=8), :],
            )
            values.append(times_conj(value, pair(turns.at[h], block(2 * g + k))))
        real, imag = from_left(
            lf,
            jnp.concatenate([values[0][0], values[1][0]], axis=1),
            jnp.concatenate([values[0][1], values[1][1]], axis=1),
        )
        for k in range(2):
            cut = slice(k * LANES, (k + 1) * LANES)
            store(mid.at[h], block(2 * g + k), (real[:, cut], imag[:, cut]))

    def stage(s, carry):
        def linear(body):
            def step(i):
                body(i // 16, span(lax.rem(i, 16) * 32, 32))

            with jax.named_scope("linear"):
                loop(32, step)

        def put(slot, h, at, value):
            store(lin.at[slot, h], at, value)

        def linear_parts():
            @pl.when(s == 1)
            def _():
                def body(h, at):
                    first = pair(nbuf.at[0, h], at)
                    value = times(pair(coef.at[QUARTER, h], at), pair(w.at[h], at))
                    less = times(pair(coef.at[HALF, h], at), first)
                    more = plus(pair(lin.at[2, h], at), times(pair(coef.at[FIRST, h], at), first))
                    put(1, h, at, minus(value, less))
                    put(2, h, at, more)

                linear(body)

            @pl.when((s == 2) | (s == 3))
            def _():
                def body(h, at):
                    more = times(pair(coef.at[SECOND, h], at), pair(nbuf.at[s - 1, h], at))
                    put(2, h, at, plus(pair(lin.at[2, h], at), more))

                linear(body)

        def columns(h):
            @pl.when(s == 0)
            def _():
                with jax.named_scope("wait_enter"):
                    wait_for(entered.at[h, pl.ds(0, (DEVICES - 1) * 8)], enter_r.at[h])

                def body(i):
                    values = []
                    for b in range(4):
                        low = entered[h, rows_of(b, i), :]
                        high = entered[h, rows_of(b + 4, i), :]
                        values.append(swap(low, high, lower_step))
                    for b in range(4):
                        store(w.at[h], rows_of(b, i), values[b])
                    open_rows(h, i, values)

                with jax.named_scope("cols"):
                    loop(128 // STEP, body)

            @pl.when(s > 0)
            def _():
                with jax.named_scope("back1"):
                    back(s - 1, 1, h)

            @pl.when((s > 0) & (s < 4))
            def _():
                base = jnp.maximum(s - 2, 0)
                scale = jnp.where(s == 3, 2.0, 1.0).astype(F32)

                def body(i):
                    values = []
                    for b, new in enumerate(closed_rows(h, i)):
                        at = rows_of(b, i)
                        more = times(pair(coef.at[HALF, h], at), (scale * new[0], scale * new[1]))
                        values.append(plus(pair(lin.at[base, h], at), more))
                        store(nbuf.at[s - 1, h], at, new)
                        store(w.at[h], at, values[-1])
                    open_rows(h, i, values)

                with jax.named_scope("cols"):
                    loop(128 // STEP, body)

            @pl.when(s == 4)
            def _():
                def body(i):
                    for b, new in enumerate(closed_rows(h, i)):
                        at = rows_of(b, i)
                        value = plus(pair(lin.at[2, h], at), times(pair(coef.at[THIRD, h], at), new))
                        first, second = swap(value[0], value[1], lower_step)
                        leaving[h, at, :] = first
                        leaving[h, rows_of(b + 4, i), :] = second

                with jax.named_scope("cols"):
                    loop(128 // STEP, body)
                for other, there in partners():
                    pltpu.make_async_remote_copy(
                        leaving.at[h, tile(other)], o_hbm.at[h, tile(me)],
                        leave_s.at[h], leave_r.at[h], device_id=there, device_id_type=MESH,
                    ).start()
                pltpu.make_async_copy(leaving.at[h, tile(me)], o_hbm.at[h, tile(me)], load_sem.at[h]).start()

            @pl.when(s < 4)
            def _():
                def send(n):
                    half, g = lax.rem(h + n, 2), (n + 1) // 2

                    @pl.when(n == 1)
                    def _():
                        linear_parts()

                    wide = pl.ds(pl.multiple_of(g * 256, 256), 256)
                    real, imag = from_left(li, tmp[half, 0:128, wide], tmp[half, 128:256, wide])
                    for k in range(2):
                        cut = slice(k * LANES, (k + 1) * LANES)
                        value = times((real[:, cut], imag[:, cut]), pair(turns.at[half], block(2 * g + k)))
                        sb1[s, g, pl.ds(half * 4 + k, 128, stride=8), :] = value[0]
                        sb1[s, g, pl.ds(half * 4 + 2 + k, 128, stride=8), :] = value[1]
                    for other, there in partners():
                        pltpu.make_async_remote_copy(
                            sb1.at[s, g, half_tile(other, half)], rb1.at[s, g, half_tile(me, half)],
                            s1.at[s, g], r1.at[s, g], device_id=there, device_id_type=MESH,
                        ).start()

                    @pl.when(half == 1)
                    def _():
                        rb1[s, g, tile(me), :] = sb1[s, g, tile(me), :]

                with jax.named_scope("sends1"):
                    loop(1 + 2 * h, send)

        loop(2, columns)

        @pl.when(s == 0)
        def _():
            with jax.named_scope("coefs1"):
                loop(64, lambda i: coefficient_table(1, i), 2)

            def body(h, at):
                value = pair(w.at[h], at)
                put(0, h, at, times(pair(coef.at[QUARTER, h], at), value))
                put(2, h, at, times(pair(coef.at[FULL, h], at), value))

            linear(body)

        def rows(g):
            with jax.named_scope("wait_rows"):
                wait_for(rb1.at[s, g, pl.ds(0, (DEVICES - 1) * 8)], r1.at[s, g])
            inner = tw[0], tw[1]

            def received(part, k):
                values = [
                    rb1[s, g, pl.ds(h * 4 + part * 2 + k, 128, stride=8), :] for h in range(2)
                ]
                return jnp.concatenate(swap(values[0], values[1], lower_tall), axis=1)

            real, imag = from_left(
                li,
                jnp.concatenate([received(0, 0), received(0, 1)], axis=1),
                jnp.concatenate([received(1, 0), received(1, 1)], axis=1),
            )
            parts = [
                times((real[:, b * LANES : (b + 1) * LANES], imag[:, b * LANES : (b + 1) * LANES]), inner)
                for b in range(4)
            ]
            real, imag = from_right(
                ri,
                jnp.concatenate([p[0] for p in parts], axis=0),
                jnp.concatenate([p[1] for p in parts], axis=0),
            )
            size = -(real * real + imag * imag)
            real, imag = size * (real - twist * imag), size * (imag + twist * real)
            real, imag = from_right(rf, real, imag)
            parts = [
                times_conj((real[b * 128 : (b + 1) * 128], imag[b * 128 : (b + 1) * 128]), inner)
                for b in range(4)
            ]
            real, imag = from_left(
                lf,
                jnp.concatenate([p[0] for p in parts], axis=1),
                jnp.concatenate([p[1] for p in parts], axis=1),
            )
            for k in range(2):
                for part, value in enumerate((real, imag)):
                    low, high = value[:, 2 * k * LANES : (2 * k + 1) * LANES], value[:, (2 * k + 1) * LANES : (2 * k + 2) * LANES]
                    for h, v in enumerate(swap(low, high, lower_tall)):
                        sb2[s, g, pl.ds(h * 4 + part * 2 + k, 128, stride=8), :] = v
            rb2[s, g, tile(me), :] = sb2[s, g, tile(me), :]

            def send(h):
                for other, there in partners():
                    pltpu.make_async_remote_copy(
                        sb2.at[s, g, half_tile(other, h)], rb2.at[s, g, half_tile(me, h)],
                        s2.at[s, g], r2.at[s, g, h], device_id=there, device_id_type=MESH,
                    ).start()

            with jax.named_scope("sends2"):
                loop(2, send)

        @pl.when(s < 4)
        def _():
            with jax.named_scope("rows"):
                loop(2, rows)
            with jax.named_scope("back0"):
                loop(2, lambda h: back(s, 0, h))

        return carry

    lax.fori_loop(0, 5, stage, 0)

    def sent(s):
        for g in range(2):
            for buffer, sem in ((sb1, s1), (sb2, s2)):
                wait_for(buffer.at[s, g, pl.ds(0, (DEVICES - 1) * 8)], sem.at[s, g])

    loop(4, sent)
    for h in range(2):
        most = packed.at[h, pl.ds(0, (DEVICES - 1) * 8)]
        wait_for(most, enter_s.at[h])
        wait_for(most, leave_s.at[h])
        pltpu.make_async_copy(leaving.at[h, tile(me)], o_hbm.at[h, tile(me)], load_sem.at[h]).wait()
        with jax.named_scope("wait_leave"):
            wait_for(most, leave_r.at[h])


def unpack_kernel(x_hbm, o_hbm, x_ref, o_ref, x_sem, o_sem):
    lower = lax.broadcasted_iota(jnp.int32, (8, LANES), 1) < 64
    tiles = DEVICES // PIECES
    into, out = [], []
    for i in range(PIECES):
        rows, lanes = pl.ds(i * tiles * 8, tiles * 8), pl.ds(i * tiles * LANES, tiles * LANES)
        into.append(pltpu.make_async_copy(x_hbm.at[:, rows], x_ref.at[:, rows], x_sem.at[i]))
        out.append(pltpu.make_async_copy(o_ref.at[:, :, lanes], o_hbm.at[:, :, lanes], o_sem.at[i]))
        into[-1].start()
    for i in range(PIECES):
        into[i].wait()
        for t in range(i * tiles, (i + 1) * tiles):
            at, lanes = slice(t * 8, t * 8 + 8), slice(t * LANES, t * LANES + LANES)
            o_ref[0, :, lanes], o_ref[1, :, lanes] = swap(x_ref[0, at, :], x_ref[1, at, :], lower)
        out[i].start()
    for copy in out:
        copy.wait()


def local(spectrum, parameters):
    hbm = pl.BlockSpec(memory_space=pl.ANY)
    field = (2, 2, ROWS // 2, LANES)
    whole = (2, ROWS, LANES)
    packed = pl.pallas_call(
        kernel,
        name="etdrk4",
        out_shape=jax.ShapeDtypeStruct(whole, F32),
        in_specs=[pl.BlockSpec(memory_space=pltpu.SMEM)] + [hbm] * 6,
        out_specs=hbm,
        scratch_shapes=[
            pltpu.VMEM(spectrum.shape, F32),
            pltpu.VMEM(whole, F32),
            pltpu.VMEM(whole, F32),
            pltpu.VMEM((256, 768), BF16),
            pltpu.VMEM((256, 768), BF16),
            pltpu.VMEM((768, 256), BF16),
            pltpu.VMEM((768, 256), BF16),
            pltpu.VMEM((2, 128, 128), F32),
            pltpu.VMEM(field, F32),
            pltpu.VMEM((2, ROWS // 2, LANES), F32),
            pltpu.VMEM((6,) + field, F32),
            pltpu.VMEM(field, F32),
            pltpu.VMEM((3,) + field, F32),
            pltpu.VMEM((3,) + field, F32),
            pltpu.VMEM((2, 256, 512), F32),
            pltpu.VMEM(field, F32),
            pltpu.VMEM(whole, F32),
        ]
        + [pltpu.VMEM((4, 2, ROWS, LANES), F32)] * 4
        + [pltpu.SemaphoreType.DMA((PIECES + 5,))]
        + [pltpu.SemaphoreType.DMA((2,))] * 4
        + [
            pltpu.SemaphoreType.DMA((4, 2)),
            pltpu.SemaphoreType.DMA((4, 2)),
            pltpu.SemaphoreType.DMA((4, 2)),
            pltpu.SemaphoreType.DMA((4, 2, 2)),
        ],
        compiler_params=pltpu.CompilerParams(
            collective_id=0, has_side_effects=True, vmem_limit_bytes=60 * 1024 * 1024
        ),
    )(
        parameters,
        spectrum,
        jnp.asarray(left_table(1.0, 1.0)),
        jnp.asarray(left_table(-1.0, 1.0)),
        jnp.asarray(right_table(1.0, NORM)),
        jnp.asarray(right_table(-1.0, NORM)),
        jnp.asarray(inner_turns()),
    )
    return pl.pallas_call(
        unpack_kernel,
        name="unpack",
        out_shape=jax.ShapeDtypeStruct(spectrum.shape, F32),
        in_specs=[hbm],
        out_specs=hbm,
        scratch_shapes=[
            pltpu.VMEM(whole, F32),
            pltpu.VMEM(spectrum.shape, F32),
            pltpu.SemaphoreType.DMA((PIECES,)),
            pltpu.SemaphoreType.DMA((PIECES,)),
        ],
        compiler_params=pltpu.CompilerParams(vmem_limit_bytes=60 * 1024 * 1024),
    )(packed)


def solution(mesh):
    return jax.shard_map(
        local,
        mesh=mesh,
        in_specs=(P(None, ("gx", "gy"), None), P()),
        out_specs=P(None, ("gx", "gy"), None),
        check_vma=False,
    )
```
